128 devices in a mesh: expert: 4 (over z), shard: 32 (over y, x, core).
Axes of the slice: x: 4, y: 4, z: 4, core: 2. Of those that a mesh axis runs over, the one named last changes fastest.
Arguments:
- tokens: bfloat16 [3072, 4096], P(('expert', 'shard')), may hold values from -0.19921875 to 0.19921875
- expert_ids: int32 [3072, 2], P(('expert', 'shard')), may hold values from 0 to 3, all different within a row; in each aligned block of 24 rows (0 to 23, 24 to 47, ...) at most 16 rows name the same one
- weight_gate: bfloat16 [4, 4096, 8192], P('expert', None, 'shard'), may hold values from -0.09375 to 0.09375
- weight_up: bfloat16 [4, 4096, 8192], P('expert', None, 'shard'), may hold values from -0.09375 to 0.09375
- gate_pre: bfloat16 [4, 2048, 8192], P('expert', None, 'shard'), may hold values from -8 to 8
- up_pre: bfloat16 [4, 2048, 8192], P('expert', None, 'shard'), may hold values from -6 to 6
- hidden_grad: bfloat16 [4, 2048, 8192], P('expert', None, 'shard'), may hold values from -6 to 6
Outputs:
- token_grad: bfloat16 [3072, 4096], P(('expert', 'shard'))
- gate_weight_grad: float32 [4, 4096, 8192], P('expert', None, 'shard')
- up_weight_grad: float32 [4, 4096, 8192], P('expert', None, 'shard')
The draws below stay inside these ranges and needn't reach their ends.
Inputs may be any that keep to these rules, and one draw needn't show every extreme that they name: `expert_ids`: each token names 2 different experts. Among the tokens of one device no expert is named more than 16 times, and in every draw some device names some expert exactly 16 times.
All inputs are finite; a program needn't handle non-finite values.
Results may differ from the reference program's by a relative error of at most 0.02.
Values may be sent and summed in bfloat16 or wider, within the bound.
A program may use at most 192 MiB of HBM per device.

```python
import math
import jax
import jax.numpy as jnp
import numpy as np
from jax import lax

D = 4096
FF = 8192
TOP = 2
TOK_DEV = 24
CAP = 16
EXPERTS = 4
TOKENS = 3072
GROUP_ROWS = 2048
N_EXPERT = 4
N_SHARD = 32


def shard_levels(rng, dims, split, smallest, high):
    loudness = 1.0
    for dim, shards_of in split:
        steps = jax.random.uniform(jax.random.fold_in(jax.random.fold_in(rng, 6), dim), (shards_of,), jnp.float32, smallest / len(split), high / len(split))
        loudness = loudness * jnp.repeat(jnp.exp(steps), dims[dim] // shards_of).reshape((-1,) + (1,) * (len(dims) - 1 - dim))
    return loudness


def shared_out(own_key, own, number, rows, amount, top, bound, slope):
    sequence = jax.random.permutation(own_key, amount)
    heavy_load, ordinary = load_shares(amount, rows * top, bound, slope, True), load_shares(amount, rows * top, bound, slope, False)
    places = jnp.arange(amount)

    def named(tallies, turn):
        used = int((tallies > 0).sum())
        fixed = max(1, used // 4)
        moved = fixed + (places - fixed + turn * (used - fixed)) % max(1, amount - fixed)
        return jnp.zeros((amount,), jnp.int32).at[sequence[jnp.where(places < fixed, places, moved)]].set(jnp.asarray(tallies, jnp.int32))

    tallies = jnp.where(number % 4 == 0, named(heavy_load, number // 4), named(ordinary, number - number // 4 - 1))
    mixed = jax.random.permutation(jax.random.fold_in(own, 3), amount)
    source_of, receiver = mixed[0:amount // 2 * 2:2], mixed[1:amount // 2 * 2:2]
    slack = jnp.minimum(tallies[source_of] - 1, bound - tallies[receiver]) // 2
    slack = jnp.where((source_of == sequence[0]) | (receiver == sequence[0]) | (tallies[receiver] == 0), 0, jnp.maximum(slack, 0))
    moved = jax.random.randint(jax.random.fold_in(own, 4), (amount // 2,), 0, 1 << 20) % (slack + 1)
    tallies = tallies.at[source_of].add(-moved).at[receiver].add(moved)
    items = jnp.searchsorted(jnp.cumsum(tallies), jnp.arange(rows * top), side="right").astype(jnp.int32)
    listing = items.reshape(top, rows).T
    listing = listing[jax.random.permutation(jax.random.fold_in(own, 1), rows)]
    turn = jax.random.randint(jax.random.fold_in(own, 2), (rows, 1), 0, top)
    return jnp.take_along_axis(listing, (jnp.arange(top)[None, :] + turn) % top, axis=1)


def load_shares(number_of, total, limit, skew, full):
    portions = [(1 << 20) // math.isqrt(standing ** skew) + 1 for standing in range(1, number_of + 1)]
    largest = limit if full else min(limit, max(-(-total // number_of), total * portions[0] // sum(portions)))
    least = 1 if total - largest >= number_of - 1 else 0
    given, surplus = [largest] + [least] * (number_of - 1), total - largest - least * (number_of - 1)
    while surplus > 0:
        free = [i for i in range(1, number_of) if given[i] < largest] or [i for i in range(1, number_of) if given[i] < limit]
        whole, budget = sum([portions[i] for i in free]), surplus
        for i in free:
            addition = min(limit - given[i], max(1, budget * portions[i] // whole), surplus)
            given[i] = given[i] + addition
            surplus = surplus - addition
    return np.array(given)


def centred(key, extent, spread, bound, pieces=(), held_as=jnp.bfloat16):
    gain = shard_levels(key, extent, pieces, -0.22, 0.18) if pieces else 1.0
    drawn = jax.random.normal(key, extent, jnp.float32) * spread * gain
    return jnp.minimum(jnp.maximum(drawn, -bound), bound).astype(held_as)


def setup_inputs(seed: int = 0) -> dict:
    streams_of = jax.random.split(jax.random.key(seed), 8)
    tokens = centred(streams_of[0], (TOKENS, D), 0.03, 0.19921875, ((0, 128),))
    expert_ids_keys = jax.random.split(jax.random.fold_in(streams_of[1], 1), TOKENS // TOK_DEV)
    expert_ids_turns = jax.random.permutation(jax.random.fold_in(streams_of[1], 3), TOKENS // TOK_DEV)
    expert_ids = jax.vmap(lambda own, number: shared_out(jax.random.fold_in(streams_of[1], 2), own, number, TOK_DEV, EXPERTS, TOP, CAP, 2))(expert_ids_keys, expert_ids_turns).reshape((TOKENS, TOP))
    weight_gate = centred(streams_of[2], (EXPERTS, D, FF), D ** -0.5, 0.09375, ((0, 4), (2, 32)))
    weight_up = centred(streams_of[3], (EXPERTS, D, FF), D ** -0.5, 0.09375, ((0, 4), (2, 32)))
    gate_pre = centred(streams_of[4], (EXPERTS, GROUP_ROWS, FF), 1.5, 8.0, ((0, 4), (2, 32)))
    up_pre = centred(streams_of[5], (EXPERTS, GROUP_ROWS, FF), 1.0, 6.0, ((0, 4), (2, 32)))
    hidden_grad = centred(streams_of[6], (EXPERTS, GROUP_ROWS, FF), 1.0, 6.0, ((0, 4), (2, 32)))
    return {"tokens": tokens, "expert_ids": expert_ids, "weight_gate": weight_gate, "weight_up": weight_up, "gate_pre": gate_pre, "up_pre": up_pre, "hidden_grad": hidden_grad}


def swiglu_grads(gate_values, up_values, hidden_cotangent):
    gate_float = gate_values.astype(jnp.float32)
    up_float = up_values.astype(jnp.float32)
    cotangent = hidden_cotangent.astype(jnp.float32)
    sigmoid_gate = jax.nn.sigmoid(gate_float)
    gate_grad = (cotangent * up_float * sigmoid_gate * (1.0 + gate_float * (1.0 - sigmoid_gate))).astype(jnp.bfloat16)
    up_grad = (cotangent * gate_float * sigmoid_gate).astype(jnp.bfloat16)
    return gate_grad, up_grad


def reference(tokens, expert_ids, weight_gate, weight_up, gate_pre, up_pre, hidden_grad):
    devices_all = N_EXPERT * N_SHARD
    width = tokens.shape[1]
    labels = jnp.arange(N_EXPERT, dtype=jnp.int32)
    one_hot = (expert_ids[:, :, None] == labels[None, None, :]).astype(jnp.int32)
    per_device = one_hot.reshape(devices_all, TOK_DEV * TOP, N_EXPERT)
    earlier = jnp.cumsum(per_device, axis=1) - per_device
    slot_index = jnp.sum(per_device * earlier, axis=2).reshape(TOKENS, TOP).astype(jnp.int32)
    token_index = jnp.arange(TOKENS, dtype=jnp.int32)
    device_index = token_index // TOK_DEV
    source_group = device_index // N_SHARD
    source_shard = device_index % N_SHARD
    row_index = ((source_shard * N_EXPERT + source_group)[:, None] * CAP + slot_index).astype(jnp.int32)
    dispatched = jnp.zeros((N_EXPERT, GROUP_ROWS, width), jnp.bfloat16)
    copies = jnp.broadcast_to(tokens[:, None, :], (TOKENS, TOP, width))
    dispatched = dispatched.at[expert_ids, row_index].set(copies)
    block_width = FF // N_SHARD
    gate_wgrads = []
    up_wgrads = []
    slot_grads = []
    for expert in range(N_EXPERT):
        gate_grad, up_grad = swiglu_grads(gate_pre[expert], up_pre[expert], hidden_grad[expert])
        rows_here = dispatched[expert]
        gate_wgrads.append(jnp.dot(rows_here.T, gate_grad, preferred_element_type=jnp.float32))
        up_wgrads.append(jnp.dot(rows_here.T, up_grad, preferred_element_type=jnp.float32))
        gate_matrix = weight_gate[expert]
        up_matrix = weight_up[expert]

        def add_block(total, block_number):
            first_unit = (block_number * block_width).astype(jnp.int32)
            gate_block = lax.dynamic_slice_in_dim(gate_grad, first_unit, block_width, 1)
            up_block = lax.dynamic_slice_in_dim(up_grad, first_unit, block_width, 1)
            gate_weights = lax.dynamic_slice_in_dim(gate_matrix, first_unit, block_width, 1)
            up_weights = lax.dynamic_slice_in_dim(up_matrix, first_unit, block_width, 1)
            block_term = jnp.dot(gate_block, gate_weights.T, preferred_element_type=jnp.float32)
            block_term = block_term + jnp.dot(up_block, up_weights.T, preferred_element_type=jnp.float32)
            return total + block_term.astype(jnp.bfloat16).astype(jnp.float32), None

        start_total = jnp.zeros((GROUP_ROWS, width), jnp.float32)
        total, unused = lax.scan(add_block, start_total, jnp.arange(N_SHARD, dtype=jnp.int32))
        slot_grads.append(total.astype(jnp.bfloat16))
    slot_all = jnp.stack(slot_grads)
    picked = slot_all[expert_ids, row_index].astype(jnp.float32)
    token_grad = jnp.sum(picked, axis=1).astype(jnp.bfloat16)
    return token_grad, jnp.stack(gate_wgrads), jnp.stack(up_wgrads)
```

```python
import functools

import jax
import jax.numpy as jnp
from jax import lax
from jax.experimental import pallas as pl
from jax.experimental.pallas import tpu as pltpu
from jax.sharding import Mesh
from jax.sharding import PartitionSpec as P

SHARD = ("shard_0", "shard_1", "shard_2")
EXPERT_SHARD = ("expert", "shard_0", "shard_1", "shard_2")
SIGN = (1, -1)
F32 = jnp.float32
BF16 = jnp.bfloat16


def shifted(value, by, size):
    return lax.rem(value + by % size, size)


def kernel(
    ids_ref, ids_t_ref, tok_ref, wg_ref, wu_ref, gate_ref, up_ref, hid_ref,
    tg_ref, og_ref, ou_ref,
    rows, grads, weights, terms, near1, far1, near2, far2, staged, pre, outgoing, returned,
    send_sem, recv_sem, local_sem, out_sem, out_send, out_recv,
):
    z = lax.axis_index("expert")
    y = lax.axis_index("shard_0")
    x = lax.axis_index("shard_1")
    c = lax.axis_index("shard_2")
    other = 1 - c
    here = y * 4 + x
    half = tok_ref.shape[1] // 2
    quarter = half // 2
    units = gate_ref.shape[2]
    tokens = tok_ref.shape[0]
    cap = 16
    part_rows = rows.shape[2] // 2

    numbers = {}

    def number(key):
        return numbers.setdefault(key, len(numbers))

    def remote(key, src, dst, device):
        i = number(key)
        return pltpu.make_async_remote_copy(
            src_ref=src,
            dst_ref=dst,
            send_sem=send_sem.at[i],
            recv_sem=recv_sem.at[i],
            device_id=device,
            device_id_type=pl.DeviceIdType.MESH,
        )

    def along(h):
        return (x, y) if h == 0 else (y, x)

    def block(h, alpha, beta):
        return beta * 4 + alpha if h == 0 else alpha * 4 + beta

    def first(h, s):
        return {"shard_1": shifted(x, SIGN[s], 4)} if h == 0 else {"shard_0": shifted(y, SIGN[s], 4)}

    def second(h, s):
        return first(1 - h, s)

    def part(p):
        return pl.ds(p * part_rows, part_rows)

    def gather1(h, s, t, arriving=False):
        alpha, beta = along(h)
        back = (1 if t == "w" else 0) + (1 if arriving else 0)
        p = 1 - s if t == "o" else s
        ref = rows.at[h, block(h, shifted(alpha, -SIGN[s] * back, 4), beta), part(p)]
        return remote(("a1", h, s, t), ref, ref, first(h, s))

    def gather2(h, s, k, t, arriving=False):
        alpha, beta = along(h)
        back = (1 if t == "w" else 0) + (1 if arriving else 0)
        p = 1 - s if t == "o" else s
        ref = rows.at[
            h, block(h, shifted(alpha, k, 4), shifted(beta, -SIGN[s] * back, 4)), part(p)
        ]
        return remote(("a2", h, s, k, t), ref, ref, second(h, s))

    def reduce1(h, s, k, t):
        alpha, beta = along(h)
        a = shifted(alpha, k, 4)
        if t == "f":
            src = terms.at[h, block(h, a, shifted(beta, 2, 4)), part(s)]
            dst = far1.at[h, s, k]
        else:
            p = 1 - s if t == "o" else s
            src = terms.at[h, block(h, a, shifted(beta, SIGN[s], 4)), part(p)]
            dst = near1.at[h, s, k, part(p)]
        return remote(("r1", h, s, k, t), src, dst, second(h, s))

    def reduce2(h, s, t):
        alpha, beta = along(h)
        if t == "f":
            src = terms.at[h, block(h, shifted(alpha, 2, 4), beta), part(s)]
            dst = far2.at[h, s]
        else:
            p = 1 - s if t == "o" else s
            src = terms.at[h, block(h, shifted(alpha, SIGN[s], 4), beta), part(p)]
            dst = near2.at[h, s, part(p)]
        return remote(("r2", h, s, t), src, dst, first(h, s))

    def slots_of(device, core):
        return pl.ds(pl.multiple_of(core * 64 + device * cap, cap), cap)

    def spread(dz, dc):
        e = shifted(z, dz, 4)
        core = shifted(c, dc, 2)
        return remote(
            ("zi", dz, dc),
            outgoing.at[core, :, pl.ds(pl.multiple_of(e * cap, cap), cap), :],
            rows.at[:, here, slots_of(z, c), :],
            {"expert": e, "shard_2": core},
        )

    def bring(dz, dc):
        j = shifted(z, dz, 4)
        core = shifted(c, dc, 2)
        return remote(
            ("zo", dz, dc),
            terms.at[:, here, slots_of(j, core), :],
            returned.at[c, :, pl.ds(pl.multiple_of(z * cap, cap), cap), :],
            {"expert": j, "shard_2": core},
        )

    partner = {"shard_2": other}

    def weight_out(which):
        ref = (wg_ref, wu_ref)[which]
        return remote(
            ("w", which),
            ref.at[0, pl.ds(pl.multiple_of(other * half, half), half), :],
            weights.at[:, pl.ds(2 * units + which * units, units)],
            partner,
        )

    def weight_in(which):
        ref = (wg_ref, wu_ref)[which]
        return pltpu.make_async_copy(
            ref.at[0, pl.ds(pl.multiple_of(c * half, half), half), :],
            weights.at[:, pl.ds(which * units, units)],
            local_sem.at[which],
        )

    def pre_in(which):
        ref = (gate_ref, up_ref, hid_ref)[which]
        return pltpu.make_async_copy(ref.at[0], pre.at[which], local_sem.at[2 + which])

    def grads_out():
        return remote(
            ("g",), grads.at[:, pl.ds(0, 2 * units)], grads.at[:, pl.ds(2 * units, 2 * units)], partner
        )

    own_in = pltpu.make_async_copy(
        outgoing.at[c, :, pl.ds(pl.multiple_of(z * cap, cap), cap), :],
        rows.at[:, here, slots_of(z, c), :],
        local_sem.at[5],
    )

    own_out = pltpu.make_async_copy(
        terms.at[:, here, slots_of(z, c), :],
        returned.at[c, :, pl.ds(pl.multiple_of(z * cap, cap), cap), :],
        local_sem.at[6],
    )

    peers = [(dz, dc) for dz in (2, 1, 3, 0) for dc in (0, 1) if (dz, dc) != (0, 0)]
    both = [(h, s) for h in (0, 1) for s in (0, 1)]

    for which in range(3):
        pre_in(which).start()
    for which in range(2):
        weight_in(which).start()
    barrier = pltpu.get_barrier_semaphore()
    for dz, dc in peers:
        pl.semaphore_signal(
            barrier, inc=1,
            device_id={"expert": shifted(z, dz, 4), "shard_2": shifted(c, dc, 2)},
            device_id_type=pl.DeviceIdType.MESH,
        )
    for h, s in both:
        pl.semaphore_signal(
            barrier, inc=1, device_id=first(h, s), device_id_type=pl.DeviceIdType.MESH
        )

    slots = 4 * cap
    expert_r = lax.broadcasted_iota(jnp.int32, (slots, tokens), 0)
    named_t = (ids_t_ref[0:1, :] == expert_r // cap) | (ids_t_ref[1:2, :] == expert_r // cap)
    before_t = (
        lax.broadcasted_iota(jnp.int32, (tokens, tokens), 0)
        < lax.broadcasted_iota(jnp.int32, (tokens, tokens), 1)
    )
    slot_t = jnp.dot(
        named_t.astype(F32).astype(BF16), before_t.astype(F32).astype(BF16),
        preferred_element_type=F32,
    )
    pick_t = jnp.where(
        named_t & (slot_t == (expert_r % cap).astype(F32)), 1.0, 0.0
    ).astype(BF16)
    for core in range(2):
        for h in range(2):
            at = core * half + h * quarter
            outgoing[core, h] = jnp.dot(
                pick_t, tok_ref[:, at:at + quarter], preferred_element_type=F32
            ).astype(BF16)

    pl.semaphore_wait(barrier, len(peers) + len(both))
    for dz, dc in peers:
        spread(dz, dc).start()
    own_in.start()
    for which in range(2):
        weight_out(which).start()

    for which in range(3):
        pre_in(which).wait()

    @pl.loop(0, pre.shape[1] // 64)
    def _(i):
        at = pl.ds(pl.multiple_of(i * 64, 64), 64)
        a = pre[0, at, :].astype(F32)
        b = pre[1, at, :].astype(F32)
        g = pre[2, at, :].astype(F32)
        sig = 1.0 / (1.0 + jnp.exp(-a))
        gs = g * sig
        grads[at, 0:units] = (gs * b * (1.0 + a * (1.0 - sig))).astype(BF16)
        grads[at, units:2 * units] = (gs * a).astype(BF16)

    grads_out().start()

    own_in.wait()
    for dz, dc in peers:
        spread(dz, dc).wait_recv()
    for t in ("f", "o"):
        for h, s in both:
            gather1(h, s, t).start()
    for t in ("f", "o"):
        for h, s in both:
            gather2(h, s, 0, t).start()

    def send_part(h, k, p):
        for s in ((0, 1) if p == 0 else (1, 0)):
            gather2(h, s, k, "f" if s == p else "o").start()

    def gather_stage(i):
        if i == 1:
            for h, s in both:
                gather1(h, s, "f", True).wait_recv()
                gather1(h, s, "w").start()
            for h in (0, 1):
                send_part(h, 3, 0)
                send_part(h, 1, 1)
        if i == 2:
            for h, s in both:
                gather1(h, s, "o", True).wait_recv()
            for h in (0, 1):
                send_part(h, 3, 1)
                send_part(h, 1, 0)
        if i == 3:
            for h, s in both:
                gather2(h, s, 0, "f", True).wait_recv()
                gather2(h, s, 0, "w").start()
        if i == 4:
            for h, s in both:
                gather1(h, s, "w", True).wait_recv()
            for h in (0, 1):
                gather2(h, 0, 2, "f").start()
                gather2(h, 1, 2, "f").start()
                gather2(h, 0, 2, "o").start()
                gather2(h, 1, 2, "o").start()
        if i == 5:
            for h in (0, 1):
                for s, k in ((0, 3), (1, 1)):
                    gather2(h, s, k, "f", True).wait_recv()
                    gather2(h, s, k, "w").start()
        if i == 6:
            for h in (0, 1):
                for s, k in ((0, 1), (1, 3)):
                    gather2(h, s, k, "f", True).wait_recv()
                    gather2(h, s, k, "w").start()

    for which in range(2):
        weight_in(which).wait()
        weight_out(which).wait_recv()
    grads_out().wait_recv()

    group = 4 * rows.shape[2]

    @pl.loop(0, 8)
    def _(i):
        for stage in range(1, 7):
            @pl.when(i == stage)
            def _():
                gather_stage(stage)
        h = i // 4
        g = i % 4

        @pl.loop(0, quarter // 256)
        def _(n):
            left = grads[pl.ds(pl.multiple_of(g * group, group), group), :]
            right = weights[pl.ds(pl.multiple_of(h * quarter + n * 256, 256), 256), :]
            out = lax.dot_general(
                left, right, (((1,), (1,)), ((), ())), preferred_element_type=F32
            ).astype(BF16)
            terms[h, pl.ds(g * 4, 4), :, pl.ds(pl.multiple_of(n * 256, 256), 256)] = out.reshape(
                4, rows.shape[2], 256
            )

    for h, s in both:
        gather2(h, s, 2, "f", True).wait_recv()
        gather2(h, s, 2, "w").start()

    for k, t in ((2, "f"), (1, "f"), (2, "o"), (3, "f")):
        for h, s in both:
            reduce1(h, s, k, t).start()

    for h, s in both:
        for k in (0, 1, 3, 2):
            gather2(h, s, k, "o", True).wait_recv()
            gather2(h, s, k, "w", True).wait_recv()

    def add_into(h, at, p, sources):
        @pl.loop(0, part_rows // 16)
        def _(i):
            lines = pl.ds(pl.multiple_of(p * part_rows + i * 16, 16), 16)
            total = terms[h, at, lines, :].astype(F32)
            for ref, base in sources:
                total = total + ref[
                    pl.ds(pl.multiple_of(base + i * 16, 16), 16), :
                ].astype(F32)
            terms[h, at, lines, :] = total.astype(BF16)

    def relay1(k):
        for h, s in both:
            reduce1(h, s, k, "f").wait_recv()
            alpha, beta = along(h)
            add_into(
                h, block(h, shifted(alpha, k, 4), shifted(beta, SIGN[s], 4)), s,
                [(far1.at[h, s, k], 0)],
            )
            reduce1(h, s, k, "w").start()

    def finish1(k):
        for h in (0, 1):
            for s in (0, 1):
                reduce1(h, s, k, "o").wait_recv()
                reduce1(h, s, k, "w").wait_recv()
            alpha, beta = along(h)
            for p in (0, 1):
                base = p * part_rows
                add_into(
                    h, block(h, shifted(alpha, k, 4), beta), p,
                    [(near1.at[h, 0, k], base), (near1.at[h, 1, k], base)],
                )

    def send1(k, t):
        for h, s in both:
            reduce1(h, s, k, t).start()

    def reduce_stage(i):
        if i == 1:
            relay1(2)
            send1(1, "o")
        if i == 2:
            relay1(1)
            send1(3, "o")
        if i == 3:
            relay1(3)
            send1(0, "f")
        if i == 4:
            finish1(2)
            for h, s in both:
                reduce2(h, s, "f").start()
            send1(0, "o")

    def out_rows(i):
        at = pl.multiple_of(c * half + i * 256, 256)
        return pl.ds(at, 256)

    def out_local(i, which):
        return pltpu.make_async_copy(
            staged.at[i, which], (og_ref, ou_ref)[which].at[0, out_rows(i), :], out_sem.at[i, which]
        )

    def out_remote(i, which):
        return pltpu.make_async_remote_copy(
            src_ref=staged.at[i, 2 + which],
            dst_ref=(og_ref, ou_ref)[which].at[0, out_rows(i), :],
            send_sem=out_send.at[i, which],
            recv_sem=out_recv.at[i, which],
            device_id=partner,
            device_id_type=pl.DeviceIdType.MESH,
        )

    all_rows = rows.shape[1] * rows.shape[2]

    @pl.loop(0, 8)
    def _(i):
        for stage in range(1, 5):
            @pl.when(i == stage)
            def _():
                reduce_stage(stage)
        h = i // 4
        m = i % 4
        left = rows[h, :, :, pl.ds(pl.multiple_of(m * 256, 256), 256)].reshape(all_rows, 256)
        for q in range(4):
            staged[i, q] = lax.dot_general(
                left, grads[:, q * units:(q + 1) * units], (((0,), (0,)), ((), ())),
                preferred_element_type=F32,
            )
        for which in range(2):
            out_local(i, which).start()
            out_remote(i, which).start()

    finish1(1)
    finish1(3)
    for h, s in both:
        reduce2(h, s, "o").start()
    relay1(0)
    for h, s in both:
        reduce2(h, s, "f").wait_recv()
        alpha, beta = along(h)
        add_into(h, block(h, shifted(alpha, SIGN[s], 4), beta), s, [(far2.at[h, s], 0)])
        reduce2(h, s, "w").start()
    finish1(0)
    for h, s in both:
        reduce2(h, s, "o").wait_recv()
        reduce2(h, s, "w").wait_recv()
    for h in (0, 1):
        for p in (0, 1):
            base = p * part_rows
            add_into(h, here, p, [(near2.at[h, 0], base), (near2.at[h, 1], base)])

    for dz, dc in peers:
        bring(dz, dc).start()
    own_out.start()

    expert_c = lax.broadcasted_iota(jnp.int32, (tokens, slots), 1)
    named = (ids_ref[:, 0:1] == expert_c // cap) | (ids_ref[:, 1:2] == expert_c // cap)
    before = (
        lax.broadcasted_iota(jnp.int32, (tokens, tokens), 1)
        < lax.broadcasted_iota(jnp.int32, (tokens, tokens), 0)
    )
    slot = jnp.dot(
        before.astype(F32).astype(BF16), named.astype(F32).astype(BF16),
        preferred_element_type=F32,
    )
    pick = jnp.where(named & (slot == (expert_c % cap).astype(F32)), 1.0, 0.0).astype(BF16)

    own_out.wait()
    for dz, dc in peers:
        bring(dz, dc).wait_recv()
    for core in range(2):
        for h in range(2):
            at = core * half + h * quarter
            tg_ref[:, at:at + quarter] = jnp.dot(
                pick, returned[core, h], preferred_element_type=F32
            ).astype(BF16)

    for dz, dc in peers:
        spread(dz, dc).wait_send()
        bring(dz, dc).wait_send()
    for which in range(2):
        weight_out(which).wait_send()
    grads_out().wait_send()
    for h, s in both:
        for t in ("f", "o", "w"):
            gather1(h, s, t).wait_send()
            reduce2(h, s, t).wait_send()
            for k in range(4):
                gather2(h, s, k, t).wait_send()
                reduce1(h, s, k, t).wait_send()

    @pl.loop(0, 8)
    def _(i):
        for which in range(2):
            out_local(i, which).wait()
            out_remote(i, which).wait()


MESSAGES = 7 + 7 + 2 + 1 + 12 + 48 + 48 + 12


def on_device(tokens, expert_ids, weight_gate, weight_up, gate_pre, up_pre, hidden_grad):
    count, width = tokens.shape
    slots, units = gate_pre.shape[1:]
    quarter = width // 4
    lines = slots // 16
    vmem = pl.BlockSpec(memory_space=pltpu.VMEM)
    anywhere = pl.BlockSpec(memory_space=pl.ANY)
    dma = pltpu.SemaphoreType.DMA
    return pl.pallas_call(
        kernel,
        out_shape=(
            jax.ShapeDtypeStruct((count, width), BF16),
            jax.ShapeDtypeStruct((1, width, units), F32),
            jax.ShapeDtypeStruct((1, width, units), F32),
        ),
        in_specs=[vmem] * 3 + [anywhere] * 5,
        out_specs=(vmem, anywhere, anywhere),
        scratch_shapes=[
            pltpu.VMEM((2, 16, lines, quarter), BF16),
            pltpu.VMEM((slots, 4 * units), BF16),
            pltpu.VMEM((2 * quarter, 4 * units), BF16),
            pltpu.VMEM((2, 16, lines, quarter), BF16),
            pltpu.VMEM((2, 2, 4, lines, quarter), BF16),
            pltpu.VMEM((2, 2, 4, lines // 2, quarter), BF16),
            pltpu.VMEM((2, 2, lines, quarter), BF16),
            pltpu.VMEM((2, 2, lines // 2, quarter), BF16),
            pltpu.VMEM((8, 4, 256, units), F32),
            pltpu.VMEM((3, slots, units), BF16),
            pltpu.VMEM((2, 2, 64, quarter), BF16),
            pltpu.VMEM((2, 2, 64, quarter), BF16),
            dma((MESSAGES,)),
            dma((MESSAGES,)),
            dma((7,)),
            dma((8, 2)),
            dma((8, 2)),
            dma((8, 2)),
        ],
        compiler_params=pltpu.CompilerParams(
            collective_id=0, has_side_effects=True, vmem_limit_bytes=60 * 1024 * 1024
        ),
    )(expert_ids, expert_ids.T, tokens, weight_gate, weight_up, gate_pre, up_pre, hidden_grad)


def solution(mesh):
    torus = Mesh(
        mesh.devices.reshape(mesh.shape["expert"], 4, 4, 2),
        ("expert", "shard_0", "shard_1", "shard_2"),
    )
    split = P("expert", None, SHARD)
    placed = (P(EXPERT_SHARD, None), P(EXPERT_SHARD, None), split, split, split, split, split)
    return jax.shard_map(
        on_device,
        mesh=torus,
        in_specs=placed,
        out_specs=(P(EXPERT_SHARD, None), split, split),
        check_vma=False,
    )
```

```python
import functools

import jax
import jax.numpy as jnp
from jax import lax
from jax.experimental import pallas as pl
from jax.experimental.pallas import tpu as pltpu
from jax.sharding import Mesh
from jax.sharding import PartitionSpec as P

SHARD = ("shard_0", "shard_1", "shard_2")
EXPERT_SHARD = ("expert", "shard_0", "shard_1", "shard_2")
SIGN = (1, -1)
F32 = jnp.float32
BF16 = jnp.bfloat16


def shifted(value, by, size):
    return lax.rem(value + by % size, size)


def picked(ids_t_ref, cap):
    tokens = ids_t_ref.shape[1]
    line = lax.broadcasted_iota(jnp.int32, (4 * cap, tokens), 0)
    named = (ids_t_ref[0:1, :] == line // cap) | (ids_t_ref[1:2, :] == line // cap)
    before = (
        lax.broadcasted_iota(jnp.int32, (tokens, tokens), 0)
        < lax.broadcasted_iota(jnp.int32, (tokens, tokens), 1)
    )
    slot = jnp.dot(
        named.astype(F32).astype(BF16), before.astype(F32).astype(BF16), preferred_element_type=F32
    )
    return jnp.where(named & (slot == (line % cap).astype(F32)), 1.0, 0.0).astype(BF16)


def finish(ids_t_ref, returned, og_in, ou_in, tg_ref, og_ref, ou_ref, sems):
    width = og_in.shape[1] // 4

    def put(i):
        which, q = i // 4, i % 4
        at = pl.ds(q * width, width)
        return pltpu.make_async_copy(
            (og_in, ou_in)[which].at[0, at, :], (og_ref, ou_ref)[which].at[0, at, :], sems.at[i]
        )

    for i in range(8):
        put(i).start()
    pick_t = picked(ids_t_ref, 16)
    quarter = returned.shape[3]
    for core in range(2):
        for h in range(2):
            at = (2 * core + h) * quarter
            tg_ref[:, at:at + quarter] = lax.dot_general(
                pick_t, returned[core, h], (((0,), (0,)), ((), ())), preferred_element_type=F32
            ).astype(BF16)
    for i in range(8):
        put(i).wait()


def kernel(
    ids_t_ref, tok_ref, wg_ref, wu_ref, gate_ref, up_ref, hid_ref,
    returned, og_ref, ou_ref,
    rows, grads, weights, terms, near1, far1, near2, far2, staged, pre, outgoing,
    send_sem, recv_sem, local_sem, out_sem, out_send, out_recv,
):
    z = lax.axis_index("expert")
    y = lax.axis_index("shard_0")
    x = lax.axis_index("shard_1")
    c = lax.axis_index("shard_2")
    other = 1 - c
    here = y * 4 + x
    half = tok_ref.shape[1] // 2
    quarter = half // 2
    units = gate_ref.shape[2]
    tokens = tok_ref.shape[0]
    cap = 16
    part_rows = rows.shape[2] // 2

    numbers = {}

    def number(key):
        return numbers.setdefault(key, len(numbers))

    def remote(key, src, dst, device):
        i = number(key)
        return pltpu.make_async_remote_copy(
            src_ref=src,
            dst_ref=dst,
            send_sem=send_sem.at[i],
            recv_sem=recv_sem.at[i],
            device_id=device,
            device_id_type=pl.DeviceIdType.MESH,
        )

    def along(h):
        return (x, y) if h == 0 else (y, x)

    def block(h, alpha, beta):
        return beta * 4 + alpha if h == 0 else alpha * 4 + beta

    def first(h, s):
        return {"shard_1": shifted(x, SIGN[s], 4)} if h == 0 else {"shard_0": shifted(y, SIGN[s], 4)}

    def second(h, s):
        return first(1 - h, s)

    def part(p):
        return pl.ds(p * part_rows, part_rows)

    def gather1(h, s, t, arriving=False):
        alpha, beta = along(h)
        back = (1 if t == "w" else 0) + (1 if arriving else 0)
        p = 1 - s if t == "o" else s
        ref = rows.at[h, block(h, shifted(alpha, -SIGN[s] * back, 4), beta), part(p)]
        return remote(("a1", h, s, t), ref, ref, first(h, s))

    def gather2(h, s, k, t, arriving=False):
        alpha, beta = along(h)
        back = (1 if t == "w" else 0) + (1 if arriving else 0)
        p = 1 - s if t == "o" else s
        ref = rows.at[
            h, block(h, shifted(alpha, k, 4), shifted(beta, -SIGN[s] * back, 4)), part(p)
        ]
        return remote(("a2", h, s, k, t), ref, ref, second(h, s))

    def reduce1(h, s, k, t):
        alpha, beta = along(h)
        a = shifted(alpha, k, 4)
        if t == "f":
            src = terms.at[h, block(h, a, shifted(beta, 2, 4)), part(s)]
            dst = far1.at[h, s, k]
        else:
            p = 1 - s if t == "o" else s
            src = terms.at[h, block(h, a, shifted(beta, SIGN[s], 4)), part(p)]
            dst = near1.at[h, s, k, part(p)]
        return remote(("r1", h, s, k, t), src, dst, second(h, s))

    def reduce2(h, s, t):
        alpha, beta = along(h)
        if t == "f":
            src = terms.at[h, block(h, shifted(alpha, 2, 4), beta), part(s)]
            dst = far2.at[h, s]
        else:
            p = 1 - s if t == "o" else s
            src = terms.at[h, block(h, shifted(alpha, SIGN[s], 4), beta), part(p)]
            dst = near2.at[h, s, part(p)]
        return remote(("r2", h, s, t), src, dst, first(h, s))

    def slots_of(device, core):
        return pl.ds(pl.multiple_of(core * 64 + device * cap, cap), cap)

    def spread(dz, dc):
        e = shifted(z, dz, 4)
        core = shifted(c, dc, 2)
        return remote(
            ("zi", dz, dc),
            outgoing.at[core, :, pl.ds(pl.multiple_of(e * cap, cap), cap), :],
            rows.at[:, here, slots_of(z, c), :],
            {"expert": e, "shard_2": core},
        )

    def bring(dz, dc):
        j = shifted(z, dz, 4)
        core = shifted(c, dc, 2)
        return remote(
            ("zo", dz, dc),
            terms.at[:, here, slots_of(j, core), :],
            returned.at[c, :, pl.ds(pl.multiple_of(z * cap, cap), cap), :],
            {"expert": j, "shard_2": core},
        )

    partner = {"shard_2": other}

    def weight_out(which):
        ref = (wg_ref, wu_ref)[which]
        return remote(
            ("w", which),
            ref.at[0, pl.ds(pl.multiple_of(other * half, half), half), :],
            weights.at[:, pl.ds(2 * units + which * units, units)],
            partner,
        )

    def weight_in(which):
        ref = (wg_ref, wu_ref)[which]
        return pltpu.make_async_copy(
            ref.at[0, pl.ds(pl.multiple_of(c * half, half), half), :],
            weights.at[:, pl.ds(which * units, units)],
            local_sem.at[which],
        )

    def pre_in(which):
        ref = (gate_ref, up_ref, hid_ref)[which]
        return pltpu.make_async_copy(ref.at[0], pre.at[which], local_sem.at[2 + which])

    def grads_out():
        return remote(
            ("g",), grads.at[:, pl.ds(0, 2 * units)], grads.at[:, pl.ds(2 * units, 2 * units)], partner
        )

    own_in = pltpu.make_async_copy(
        outgoing.at[c, :, pl.ds(pl.multiple_of(z * cap, cap), cap), :],
        rows.at[:, here, slots_of(z, c), :],
        local_sem.at[5],
    )

    own_out = pltpu.make_async_copy(
        terms.at[:, here, slots_of(z, c), :],
        returned.at[c, :, pl.ds(pl.multiple_of(z * cap, cap), cap), :],
        local_sem.at[6],
    )

    peers = [(dz, dc) for dz in (2, 1, 3, 0) for dc in (0, 1) if (dz, dc) != (0, 0)]
    both = [(h, s) for h in (0, 1) for s in (0, 1)]

    for which in range(3):
        pre_in(which).start()
    for which in range(2):
        weight_in(which).start()
    barrier = pltpu.get_barrier_semaphore()
    for dz, dc in peers:
        pl.semaphore_signal(
            barrier, inc=1,
            device_id={"expert": shifted(z, dz, 4), "shard_2": shifted(c, dc, 2)},
            device_id_type=pl.DeviceIdType.MESH,
        )
    for h, s in both:
        pl.semaphore_signal(
            barrier, inc=1, device_id=first(h, s), device_id_type=pl.DeviceIdType.MESH
        )

    pick_t = picked(ids_t_ref, cap)
    for core in range(2):
        for h in range(2):
            at = core * half + h * quarter
            outgoing[core, h] = jnp.dot(
                pick_t, tok_ref[:, at:at + quarter], preferred_element_type=F32
            ).astype(BF16)

    pl.semaphore_wait(barrier, len(peers) + len(both))
    for dz, dc in peers:
        spread(dz, dc).start()
    own_in.start()
    for which in range(2):
        weight_out(which).start()

    for which in range(3):
        pre_in(which).wait()

    @pl.loop(0, pre.shape[1] // 64)
    def _(i):
        at = pl.ds(pl.multiple_of(i * 64, 64), 64)
        a = pre[0, at, :].astype(F32)
        b = pre[1, at, :].astype(F32)
        g = pre[2, at, :].astype(F32)
        sig = 1.0 / (1.0 + jnp.exp(-a))
        gs = g * sig
        grads[at, 0:units] = (gs * b * (1.0 + a * (1.0 - sig))).astype(BF16)
        grads[at, units:2 * units] = (gs * a).astype(BF16)

    grads_out().start()

    own_in.wait()
    for dz, dc in peers:
        spread(dz, dc).wait_recv()
    for t in ("f", "o"):
        for h, s in both:
            gather1(h, s, t).start()
    for t in ("f", "o"):
        for h, s in both:
            gather2(h, s, 0, t).start()

    def send_part(h, k, p):
        for s in ((0, 1) if p == 0 else (1, 0)):
            gather2(h, s, k, "f" if s == p else "o").start()

    def gather_stage(i):
        if i == 1:
            for h, s in both:
                gather1(h, s, "f", True).wait_recv()
                gather1(h, s, "w").start()
            for h in (0, 1):
                send_part(h, 3, 0)
                send_part(h, 1, 1)
        if i == 2:
            for h, s in both:
                gather1(h, s, "o", True).wait_recv()
            for h in (0, 1):
                send_part(h, 3, 1)
                send_part(h, 1, 0)
        if i == 3:
            for h, s in both:
                gather2(h, s, 0, "f", True).wait_recv()
                gather2(h, s, 0, "w").start()
        if i == 4:
            for h, s in both:
                gather1(h, s, "w", True).wait_recv()
            for h in (0, 1):
                gather2(h, 0, 2, "f").start()
                gather2(h, 1, 2, "f").start()
                gather2(h, 0, 2, "o").start()
                gather2(h, 1, 2, "o").start()
        if i == 5:
            for h in (0, 1):
                for s, k in ((0, 3), (1, 1)):
                    gather2(h, s, k, "f", True).wait_recv()
                    gather2(h, s, k, "w").start()
        if i == 6:
            for h in (0, 1):
                for s, k in ((0, 1), (1, 3)):
                    gather2(h, s, k, "f", True).wait_recv()
                    gather2(h, s, k, "w").start()

    for which in range(2):
        weight_in(which).wait()
        weight_out(which).wait_recv()
    grads_out().wait_recv()

    group = 4 * rows.shape[2]

    @pl.loop(0, 8)
    def _(i):
        for stage in range(1, 7):
            @pl.when(i == stage)
            def _():
                gather_stage(stage)
        h = i // 4
        g = i % 4

        @pl.loop(0, quarter // 256)
        def _(n):
            left = grads[pl.ds(pl.multiple_of(g * group, group), group), :]
            right = weights[pl.ds(pl.multiple_of(h * quarter + n * 256, 256), 256), :]
            out = lax.dot_general(
                left, right, (((1,), (1,)), ((), ())), preferred_element_type=F32
            ).astype(BF16)
            terms[h, pl.ds(g * 4, 4), :, pl.ds(pl.multiple_of(n * 256, 256), 256)] = out.reshape(
                4, rows.shape[2], 256
            )

    for h, s in both:
        gather2(h, s, 2, "f", True).wait_recv()
        gather2(h, s, 2, "w").start()

    for k, t in ((2, "f"), (1, "f"), (2, "o"), (3, "f")):
        for h, s in both:
            reduce1(h, s, k, t).start()

    for h, s in both:
        for k in (0, 1, 3, 2):
            gather2(h, s, k, "o", True).wait_recv()
            gather2(h, s, k, "w", True).wait_recv()

    def add_into(h, at, p, sources):
        @pl.loop(0, part_rows // 16)
        def _(i):
            lines = pl.ds(pl.multiple_of(p * part_rows + i * 16, 16), 16)
            total = terms[h, at, lines, :].astype(F32)
            for ref, base in sources:
                total = total + ref[
                    pl.ds(pl.multiple_of(base + i * 16, 16), 16), :
                ].astype(F32)
            terms[h, at, lines, :] = total.astype(BF16)

    def relay1(k):
        for h, s in both:
            reduce1(h, s, k, "f").wait_recv()
            alpha, beta = along(h)
            add_into(
                h, block(h, shifted(alpha, k, 4), shifted(beta, SIGN[s], 4)), s,
                [(far1.at[h, s, k], 0)],
            )
            reduce1(h, s, k, "w").start()

    def finish1(k):
        for h in (0, 1):
            for s in (0, 1):
                reduce1(h, s, k, "o").wait_recv()
                reduce1(h, s, k, "w").wait_recv()
            alpha, beta = along(h)
            for p in (0, 1):
                base = p * part_rows
                add_into(
                    h, block(h, shifted(alpha, k, 4), beta), p,
                    [(near1.at[h, 0, k], base), (near1.at[h, 1, k], base)],
                )

    def send1(k, t):
        for h, s in both:
            reduce1(h, s, k, t).start()

    def reduce_stage(i):
        if i == 1:
            relay1(2)
            send1(1, "o")
        if i == 2:
            relay1(1)
            send1(3, "o")
        if i == 3:
            relay1(3)
            send1(0, "f")
        if i == 4:
            finish1(2)
            for h, s in both:
                reduce2(h, s, "f").start()
            send1(0, "o")

    def out_rows(i):
        at = pl.multiple_of(c * half + i * 256, 256)
        return pl.ds(at, 256)

    def out_local(i, which):
        return pltpu.make_async_copy(
            staged.at[i, which], (og_ref, ou_ref)[which].at[0, out_rows(i), :], out_sem.at[i, which]
        )

    def out_remote(i, which):
        return pltpu.make_async_remote_copy(
            src_ref=staged.at[i, 2 + which],
            dst_ref=(og_ref, ou_ref)[which].at[0, out_rows(i), :],
            send_sem=out_send.at[i, which],
            recv_sem=out_recv.at[i, which],
            device_id=partner,
            device_id_type=pl.DeviceIdType.MESH,
        )

    all_rows = rows.shape[1] * rows.shape[2]

    @pl.loop(0, 8)
    def _(i):
        for stage in range(1, 5):
            @pl.when(i == stage)
            def _():
                reduce_stage(stage)
        h = i // 4
        m = i % 4
        left = rows[h, :, :, pl.ds(pl.multiple_of(m * 256, 256), 256)].reshape(all_rows, 256)
        for q in range(4):
            staged[i, q] = lax.dot_general(
                left, grads[:, q * units:(q + 1) * units], (((0,), (0,)), ((), ())),
                preferred_element_type=F32,
            )
        for which in range(2):
            out_local(i, which).start()
            out_remote(i, which).start()

    finish1(1)
    finish1(3)
    for h, s in both:
        reduce2(h, s, "o").start()
    relay1(0)
    for h, s in both:
        reduce2(h, s, "f").wait_recv()
        alpha, beta = along(h)
        add_into(h, block(h, shifted(alpha, SIGN[s], 4), beta), s, [(far2.at[h, s], 0)])
        reduce2(h, s, "w").start()
    finish1(0)
    for h, s in both:
        reduce2(h, s, "o").wait_recv()
        reduce2(h, s, "w").wait_recv()
    for h in (0, 1):
        for p in (0, 1):
            base = p * part_rows
            add_into(h, here, p, [(near2.at[h, 0], base), (near2.at[h, 1], base)])

    for dz, dc in peers:
        bring(dz, dc).start()
    own_out.start()

    own_out.wait()
    for dz, dc in peers:
        bring(dz, dc).wait_recv()
    for dz, dc in peers:
        spread(dz, dc).wait_send()
        bring(dz, dc).wait_send()
    for which in range(2):
        weight_out(which).wait_send()
    grads_out().wait_send()
    for h, s in both:
        for t in ("f", "o", "w"):
            gather1(h, s, t).wait_send()
            reduce2(h, s, t).wait_send()
            for k in range(4):
                gather2(h, s, k, t).wait_send()
                reduce1(h, s, k, t).wait_send()

    @pl.loop(0, 8)
    def _(i):
        for which in range(2):
            out_local(i, which).wait()
            out_remote(i, which).wait()


MESSAGES = 7 + 7 + 2 + 1 + 12 + 48 + 48 + 12


def on_device(tokens, expert_ids, weight_gate, weight_up, gate_pre, up_pre, hidden_grad):
    count, width = tokens.shape
    slots, units = gate_pre.shape[1:]
    quarter = width // 4
    lines = slots // 16
    vmem = pl.BlockSpec(memory_space=pltpu.VMEM)
    anywhere = pl.BlockSpec(memory_space=pl.ANY)
    dma = pltpu.SemaphoreType.DMA
    ids_t = expert_ids.T
    returned, gate_out, up_out = pl.pallas_call(
        kernel,
        out_shape=(
            pltpu.VMEM((2, 2, 64, quarter), BF16),
            pltpu.VMEM((1, width, units), F32),
            pltpu.VMEM((1, width, units), F32),
        ),
        in_specs=[vmem] * 2 + [anywhere] * 5,
        out_specs=(anywhere, anywhere, anywhere),
        scratch_shapes=[
            pltpu.VMEM((2, 16, lines, quarter), BF16),
            pltpu.VMEM((slots, 4 * units), BF16),
            pltpu.VMEM((2 * quarter, 4 * units), BF16),
            pltpu.VMEM((2, 16, lines, quarter), BF16),
            pltpu.VMEM((2, 2, 4, lines, quarter), BF16),
            pltpu.VMEM((2, 2, 4, lines // 2, quarter), BF16),
            pltpu.VMEM((2, 2, lines, quarter), BF16),
            pltpu.VMEM((2, 2, lines // 2, quarter), BF16),
            pltpu.VMEM((8, 4, 256, units), F32),
            pltpu.VMEM((3, slots, units), BF16),
            pltpu.VMEM((2, 2, 64, quarter), BF16),
            dma((MESSAGES,)),
            dma((MESSAGES,)),
            dma((7,)),
            dma((8, 2)),
            dma((8, 2)),
            dma((8, 2)),
        ],
        compiler_params=pltpu.CompilerParams(
            collective_id=0, has_side_effects=True, vmem_limit_bytes=46 * 1024 * 1024
        ),
    )(ids_t, tokens, weight_gate, weight_up, gate_pre, up_pre, hidden_grad)
    return pl.pallas_call(
        finish,
        out_shape=(
            jax.ShapeDtypeStruct((count, width), BF16),
            jax.ShapeDtypeStruct((1, width, units), F32),
            jax.ShapeDtypeStruct((1, width, units), F32),
        ),
        in_specs=[vmem, vmem, anywhere, anywhere],
        out_specs=(vmem, anywhere, anywhere),
        scratch_shapes=[dma((8,))],
        compiler_params=pltpu.CompilerParams(vmem_limit_bytes=8 * 1024 * 1024),
    )(ids_t, returned, gate_out, up_out)


def solution(mesh):
    torus = Mesh(
        mesh.devices.reshape(mesh.shape["expert"], 4, 4, 2),
        ("expert", "shard_0", "shard_1", "shard_2"),
    )
    split = P("expert", None, SHARD)
    placed = (P(EXPERT_SHARD, None), P(EXPERT_SHARD, None), split, split, split, split, split)
    return jax.shard_map(
        on_device,
        mesh=torus,
        in_specs=placed,
        out_specs=(P(EXPERT_SHARD, None), split, split),
        check_vma=False,
    )
```

```python
import functools

import jax
import jax.numpy as jnp
from jax import lax
from jax.experimental import pallas as pl
from jax.experimental.pallas import tpu as pltpu
from jax.sharding import Mesh
from jax.sharding import PartitionSpec as P

SHARD = ("shard_0", "shard_1", "shard_2")
EXPERT_SHARD = ("expert", "shard_0", "shard_1", "shard_2")
SIGN = (1, -1)
F32 = jnp.float32
BF16 = jnp.bfloat16


def shifted(value, by, size):
    return lax.rem(value + by % size, size)


def picked(first_ids, second_ids, cap):
    tokens = first_ids.shape[1]
    line = lax.broadcasted_iota(jnp.int32, (4 * cap, tokens), 0)
    expert = (line // cap).astype(F32)
    named = (first_ids == expert) | (second_ids == expert)
    before = (
        lax.broadcasted_iota(jnp.int32, (tokens, tokens), 0)
        < lax.broadcasted_iota(jnp.int32, (tokens, tokens), 1)
    )
    slot = jnp.dot(
        named.astype(F32).astype(BF16), before.astype(F32).astype(BF16), preferred_element_type=F32
    )
    return jnp.where(named & (slot == (line % cap).astype(F32)), 1.0, 0.0).astype(BF16)


def finish(ids_t_ref, returned, summed, og_in, ou_in, tg_ref, og_ref, ou_ref, sems):
    width = og_in.shape[1] // 4

    def put(i):
        which, q = i // 4, i % 4
        at = pl.ds(q * width, width)
        return pltpu.make_async_copy(
            (og_in, ou_in)[which].at[0, at, :], (og_ref, ou_ref)[which].at[0, at, :], sems.at[i]
        )

    for i in range(8):
        put(i).start()
    ids = ids_t_ref[...].astype(F32)
    pick_t = picked(ids[0:1, :], ids[1:2, :], 16)
    tokens = tg_ref.shape[0]
    half = tg_ref.shape[1] // 2
    quarter = returned.shape[3]
    for core in range(2):
        for h in range(2):
            at = core * half + h * quarter
            tg_ref[:, at:at + quarter] = lax.dot_general(
                pick_t, returned[core, h], (((0,), (0,)), ((), ())), preferred_element_type=F32
            ).astype(BF16)
        at = core * half + 2 * quarter
        tg_ref[:, at:(core + 1) * half] = summed[core, 0:tokens, :]
    for i in range(8):
        put(i).wait()


def kernel(
    ids_t_ref, tok_ref, wg_ref, wu_ref, gate_ref, up_ref, hid_ref,
    returned, summed, og_ref, ou_ref,
    rows, rows_f, grads, weights, terms, terms_f, near1, far1, near2, far2, staged, pre, outgoing,
    block_f, plane_f, slots_f, crossed_f, totals_f, sums1_f, sums2_f, last_f,
    send_sem, recv_sem, local_sem, out_sem, out_send, out_recv,
):
    z = lax.axis_index("expert")
    y = lax.axis_index("shard_0")
    x = lax.axis_index("shard_1")
    c = lax.axis_index("shard_2")
    other = 1 - c
    here = y * 4 + x
    half = tok_ref.shape[1] // 2
    quarter = rows.shape[3]
    wide_f = rows_f.shape[5]
    units = gate_ref.shape[2]
    tokens = tok_ref.shape[0]
    cap = 16
    part_rows = rows.shape[2] // 2

    numbers = {}

    def number(key):
        return numbers.setdefault(key, len(numbers))

    def remote(key, src, dst, device):
        i = number(key)
        return pltpu.make_async_remote_copy(
            src_ref=src,
            dst_ref=dst,
            send_sem=send_sem.at[i],
            recv_sem=recv_sem.at[i],
            device_id=device,
            device_id_type=pl.DeviceIdType.MESH,
        )

    def along(h):
        return (x, y) if h == 0 else (y, x)

    def block(h, alpha, beta):
        return beta * 4 + alpha if h == 0 else alpha * 4 + beta

    def first(h, s):
        return {"shard_1": shifted(x, SIGN[s], 4)} if h == 0 else {"shard_0": shifted(y, SIGN[s], 4)}

    def second(h, s):
        return first(1 - h, s)

    def part(p):
        return pl.ds(p * part_rows, part_rows)

    def gather1(h, s, t, arriving=False):
        alpha, beta = along(h)
        back = (1 if t == "w" else 0) + (1 if arriving else 0)
        p = 1 - s if t == "o" else s
        ref = rows.at[h, block(h, shifted(alpha, -SIGN[s] * back, 4), beta), part(p)]
        return remote(("a1", h, s, t), ref, ref, first(h, s))

    def gather2(h, s, k, t, arriving=False):
        alpha, beta = along(h)
        back = (1 if t == "w" else 0) + (1 if arriving else 0)
        p = 1 - s if t == "o" else s
        ref = rows.at[
            h, block(h, shifted(alpha, k, 4), shifted(beta, -SIGN[s] * back, 4)), part(p)
        ]
        return remote(("a2", h, s, k, t), ref, ref, second(h, s))

    def reduce1(h, s, k, t):
        alpha, beta = along(h)
        a = shifted(alpha, k, 4)
        if t == "f":
            src = terms.at[h, block(h, a, shifted(beta, 2, 4)), part(s)]
            dst = far1.at[h, s, k]
        else:
            p = 1 - s if t == "o" else s
            src = terms.at[h, block(h, a, shifted(beta, SIGN[s], 4)), part(p)]
            dst = near1.at[h, s, k, part(p)]
        return remote(("r1", h, s, k, t), src, dst, second(h, s))

    def reduce2(h, s, t):
        alpha, beta = along(h)
        if t == "f":
            src = terms.at[h, block(h, shifted(alpha, 2, 4), beta), part(s)]
            dst = far2.at[h, s]
        else:
            p = 1 - s if t == "o" else s
            src = terms.at[h, block(h, shifted(alpha, SIGN[s], 4), beta), part(p)]
            dst = near2.at[h, s, part(p)]
        return remote(("r2", h, s, t), src, dst, first(h, s))

    def slots_of(device, core):
        return pl.ds(pl.multiple_of(core * 64 + device * cap, cap), cap)

    def spread(dz, dc):
        e = shifted(z, dz, 4)
        core = shifted(c, dc, 2)
        return remote(
            ("zi", dz, dc),
            outgoing.at[core, :, pl.ds(pl.multiple_of(e * cap, cap), cap), :],
            rows.at[:, here, slots_of(z, c), :],
            {"expert": e, "shard_2": core},
        )

    def bring(dz, dc):
        j = shifted(z, dz, 4)
        core = shifted(c, dc, 2)
        return remote(
            ("zo", dz, dc),
            terms.at[:, here, slots_of(j, core), :],
            returned.at[c, :, pl.ds(pl.multiple_of(z * cap, cap), cap), :],
            {"expert": j, "shard_2": core},
        )

    partner = {"shard_2": other}

    def aside1(h, o):
        return {"shard_1": shifted(x, o, 4)} if h == 0 else {"shard_0": shifted(y, o, 4)}

    def aside2(h, o):
        return aside1(1 - h, o)

    def block_out():
        return remote(
            ("fb",), block_f.at[other], plane_f.at[c, here * (1 - c) + (x * 4 + y) * c], partner
        )

    block_own = pltpu.make_async_copy(
        block_f.at[c], plane_f.at[c, here * (1 - c) + (x * 4 + y) * c], local_sem.at[7]
    )

    def plane1(h, o):
        alpha, beta = along(h)
        ref = plane_f.at[h, beta * 4 + alpha]
        return remote(("f1", h, o), ref, ref, aside1(h, o))

    def plane2(h, o):
        alpha, beta = along(h)
        ref = plane_f.at[h, pl.ds(beta * 4, 4)]
        return remote(("f2", h, o), ref, ref, aside2(h, o))

    def group_rows(h, at, j):
        return rows_f.at[at, :, 0, j] if h == 0 else rows_f.at[:, at, 1, j]

    TURN = (0, 1, 3, 2)

    def slots_out(h, n, dz):
        e = shifted(z, dz, 4)
        at = shifted(along(h)[1], TURN[n], 4)
        return remote(
            ("fz", h, n, dz),
            slots_f.at[h, n, :, pl.ds(pl.multiple_of(e * cap, cap), cap), :],
            group_rows(h, at, z),
            {"expert": e},
        )

    def slots_own(h, n):
        at = shifted(along(h)[1], TURN[n], 4)
        return pltpu.make_async_copy(
            slots_f.at[h, n, :, pl.ds(pl.multiple_of(z * cap, cap), cap), :],
            group_rows(h, at, z),
            local_sem.at[8 + h * 4 + n],
        )

    def picked_of(h, at):
        ids = plane_f[h, at, tokens:tokens + 8, 0:128].astype(F32)
        lines = plane_f.shape[2]
        return picked(ids[0:1, 0:lines], ids[1:2, 0:lines], cap)

    def make_slots(h, n):
        at = shifted(along(h)[1], TURN[n], 4)

        @pl.loop(0, 4)
        def _(i):
            slots_f[h, n, i] = jnp.dot(
                picked_of(h, at * 4 + i), plane_f[h, at * 4 + i], preferred_element_type=F32
            ).astype(BF16)

        for dz in (2, 1, 3):
            slots_out(h, n, dz).start()
        slots_own(h, n).start()

    def terms_out(g, dz):
        j = shifted(z, dz, 4)
        return remote(
            ("ft", g, dz), terms_f.at[g, :, :, j], crossed_f.at[z, g], {"expert": j}
        )

    terms_own = pltpu.make_async_copy(terms_f.at[:, :, :, z], crossed_f.at[z], local_sem.at[16])

    def make_totals():
        for h in (0, 1):
            @pl.loop(0, 16)
            def _(i):
                one, two = i // 4, i % 4
                held = crossed_f[:, one, two, 0] if h == 0 else crossed_f[:, two, one, 1]
                totals_f[h, i] = lax.dot_general(
                    picked_of(h, i), held.reshape(4 * cap, wide_f), (((0,), (0,)), ((), ())),
                    preferred_element_type=F32,
                ).astype(BF16)

    def back1(h, o):
        alpha, beta = along(h)
        return remote(
            ("b1", h, o), totals_f.at[h, pl.ds(shifted(beta, o, 4) * 4, 4)],
            sums1_f.at[h, o - 1], aside2(h, o),
        )

    def back2(h, o):
        alpha, beta = along(h)
        return remote(
            ("b2", h, o), totals_f.at[h, beta * 4 + shifted(alpha, o, 4)],
            sums2_f.at[h, o - 1], aside1(h, o),
        )

    def last_out():
        return remote(("fl",), last_f.at[other], summed.at[c], partner)

    last_own = pltpu.make_async_copy(last_f.at[c], summed.at[c], local_sem.at[17])
    around = [(h, o) for o in (2, 1, 3) for h in (0, 1)]

    def weight_out(which):
        ref = (wg_ref, wu_ref)[which]
        return remote(
            ("w", which),
            ref.at[0, pl.ds(pl.multiple_of(other * half, half), half), :],
            weights.at[:, pl.ds(2 * units + which * units, units)],
            partner,
        )

    def weight_in(which):
        ref = (wg_ref, wu_ref)[which]
        return pltpu.make_async_copy(
            ref.at[0, pl.ds(pl.multiple_of(c * half, half), half), :],
            weights.at[:, pl.ds(which * units, units)],
            local_sem.at[which],
        )

    def pre_in(which):
        ref = (gate_ref, up_ref, hid_ref)[which]
        return pltpu.make_async_copy(ref.at[0], pre.at[which], local_sem.at[2 + which])

    def grads_out():
        return remote(
            ("g",), grads.at[:, pl.ds(0, 2 * units)], grads.at[:, pl.ds(2 * units, 2 * units)], partner
        )

    own_in = pltpu.make_async_copy(
        outgoing.at[c, :, pl.ds(pl.multiple_of(z * cap, cap), cap), :],
        rows.at[:, here, slots_of(z, c), :],
        local_sem.at[5],
    )

    own_out = pltpu.make_async_copy(
        terms.at[:, here, slots_of(z, c), :],
        returned.at[c, :, pl.ds(pl.multiple_of(z * cap, cap), cap), :],
        local_sem.at[6],
    )

    peers = [(dz, dc) for dz in (2, 1, 3, 0) for dc in (0, 1) if (dz, dc) != (0, 0)]
    both = [(h, s) for h in (0, 1) for s in (0, 1)]

    for which in range(3):
        pre_in(which).start()
    for which in range(2):
        weight_in(which).start()
    barrier = pltpu.get_barrier_semaphore()
    for dz, dc in peers:
        pl.semaphore_signal(
            barrier, inc=1,
            device_id={"expert": shifted(z, dz, 4), "shard_2": shifted(c, dc, 2)},
            device_id_type=pl.DeviceIdType.MESH,
        )
    for h, s in both:
        pl.semaphore_signal(
            barrier, inc=1, device_id=first(h, s), device_id_type=pl.DeviceIdType.MESH
        )
    for h in (0, 1):
        pl.semaphore_signal(
            barrier, inc=1, device_id=aside1(h, 2), device_id_type=pl.DeviceIdType.MESH
        )

    ids = ids_t_ref[...].astype(F32)
    pick_t = picked(ids[0:1, :], ids[1:2, :], cap)
    for core in range(2):
        at = core * half + 2 * quarter
        block_f[core, 0:tokens, :] = tok_ref[:, at:at + wide_f]
        block_f[core, tokens:, :] = jnp.full((block_f.shape[1] - tokens, wide_f), 9.0, BF16)
        block_f[core, tokens:tokens + 2, 0:tokens] = ids.astype(BF16)
    for core in range(2):
        for h in range(2):
            at = core * half + h * quarter
            outgoing[core, h] = jnp.dot(
                pick_t, tok_ref[:, at:at + quarter], preferred_element_type=F32
            ).astype(BF16)

    pl.semaphore_wait(barrier, len(peers) + len(both) + 2)
    block_out().start()
    block_own.start()
    for dz, dc in peers:
        spread(dz, dc).start()
    own_in.start()
    for which in range(2):
        weight_out(which).start()

    block_own.wait()
    block_out().wait_recv()
    for h, o in around:
        plane1(h, o).start()

    for which in range(3):
        pre_in(which).wait()

    @pl.loop(0, pre.shape[1] // 64)
    def _(i):
        at = pl.ds(pl.multiple_of(i * 64, 64), 64)
        a = pre[0, at, :].astype(F32)
        b = pre[1, at, :].astype(F32)
        g = pre[2, at, :].astype(F32)
        sig = 1.0 / (1.0 + jnp.exp(-a))
        gs = g * sig
        grads[at, 0:units] = (gs * b * (1.0 + a * (1.0 - sig))).astype(BF16)
        grads[at, units:2 * units] = (gs * a).astype(BF16)

    grads_out().start()

    own_in.wait()
    for dz, dc in peers:
        spread(dz, dc).wait_recv()
    for t in ("f", "o"):
        for h, s in both:
            gather1(h, s, t).start()
    for h, o in around:
        plane1(h, o).wait_recv()
    for h, o in around:
        plane2(h, o).start()
    for t in ("f", "o"):
        for h, s in both:
            gather2(h, s, 0, t).start()

    def send_part(h, k, p):
        for s in ((0, 1) if p == 0 else (1, 0)):
            gather2(h, s, k, "f" if s == p else "o").start()

    def group_stage(n):
        for h in (0, 1):
            if n:
                plane2(h, (None, 3, 1, 2)[n]).wait_recv()
            make_slots(h, n)

    def gather_stage(i):
        if i == 0:
            group_stage(0)
        if i == 1:
            for h, s in both:
                gather1(h, s, "f", True).wait_recv()
                gather1(h, s, "w").start()
            for h in (0, 1):
                send_part(h, 3, 0)
                send_part(h, 1, 1)
        if i == 2:
            for h, s in both:
                gather1(h, s, "o", True).wait_recv()
            for h in (0, 1):
                send_part(h, 3, 1)
                send_part(h, 1, 0)
            for g in range(4):
                for dz in (2, 1, 3):
                    terms_out(g, dz).start()
            terms_own.start()
        if i == 3:
            for h, s in both:
                gather2(h, s, 0, "f", True).wait_recv()
                gather2(h, s, 0, "w").start()
            group_stage(1)
        if i == 4:
            for h, s in both:
                gather1(h, s, "w", True).wait_recv()
            for h in (0, 1):
                gather2(h, 0, 2, "f").start()
                gather2(h, 1, 2, "f").start()
                gather2(h, 0, 2, "o").start()
                gather2(h, 1, 2, "o").start()
            group_stage(2)
        if i == 5:
            for h in (0, 1):
                for s, k in ((0, 3), (1, 1)):
                    gather2(h, s, k, "f", True).wait_recv()
                    gather2(h, s, k, "w").start()
            group_stage(3)
        if i == 6:
            for h in (0, 1):
                for s, k in ((0, 1), (1, 3)):
                    gather2(h, s, k, "f", True).wait_recv()
                    gather2(h, s, k, "w").start()

    for which in range(2):
        weight_in(which).wait()
        weight_out(which).wait_recv()
    grads_out().wait_recv()

    group = 4 * rows.shape[2]

    @pl.loop(0, 8)
    def _(i):
        for stage in range(7):
            @pl.when(i == stage)
            def _():
                gather_stage(stage)
        tile = (i + 6) % 8

        @pl.loop(0, 4)
        def _(g):
            left = grads[pl.ds(pl.multiple_of(g * group, group), group), :]
            right = weights[pl.ds(pl.multiple_of(tile * 256, 256), 256), :]
            out = lax.dot_general(
                left, right, (((1,), (1,)), ((), ())), preferred_element_type=F32
            ).astype(BF16)

            @pl.when(tile < 6)
            def _():
                terms[
                    tile // 3, pl.ds(g * 4, 4), :, pl.ds(pl.multiple_of(tile % 3 * 256, 256), 256)
                ] = out.reshape(4, rows.shape[2], 256)

            for m in range(2):
                @pl.when(tile == 6 + m)
                def _():
                    terms_f[g, :, :, :, :, m * 256:(m + 1) * 256] = out.reshape(4, 2, 4, cap, 256)

    for h, s in both:
        gather2(h, s, 2, "f", True).wait_recv()
        gather2(h, s, 2, "w").start()

    for k, t in ((2, "f"), (1, "f"), (2, "o"), (3, "f")):
        for h, s in both:
            reduce1(h, s, k, t).start()

    for h, s in both:
        for k in (0, 1, 3, 2):
            gather2(h, s, k, "o", True).wait_recv()
            gather2(h, s, k, "w", True).wait_recv()

    def add_into(h, at, p, sources):
        @pl.loop(0, part_rows // 16)
        def _(i):
            lines = pl.ds(pl.multiple_of(p * part_rows + i * 16, 16), 16)
            total = terms[h, at, lines, :].astype(F32)
            for ref, base in sources:
                total = total + ref[
                    pl.ds(pl.multiple_of(base + i * 16, 16), 16), :
                ].astype(F32)
            terms[h, at, lines, :] = total.astype(BF16)

    def relay1(k):
        for h, s in both:
            reduce1(h, s, k, "f").wait_recv()
            alpha, beta = along(h)
            add_into(
                h, block(h, shifted(alpha, k, 4), shifted(beta, SIGN[s], 4)), s,
                [(far1.at[h, s, k], 0)],
            )
            reduce1(h, s, k, "w").start()

    def finish1(k):
        for h in (0, 1):
            for s in (0, 1):
                reduce1(h, s, k, "o").wait_recv()
                reduce1(h, s, k, "w").wait_recv()
            alpha, beta = along(h)
            for p in (0, 1):
                base = p * part_rows
                add_into(
                    h, block(h, shifted(alpha, k, 4), beta), p,
                    [(near1.at[h, 0, k], base), (near1.at[h, 1, k], base)],
                )

    def send1(k, t):
        for h, s in both:
            reduce1(h, s, k, t).start()

    def reduce_stage(i):
        if i == 1:
            relay1(2)
            send1(1, "o")
        if i == 2:
            relay1(1)
            send1(3, "o")
        if i == 3:
            relay1(3)
            send1(0, "f")
        if i == 4:
            finish1(2)
            for h, s in both:
                reduce2(h, s, "f").start()
            send1(0, "o")

    def out_rows(i):
        at = pl.multiple_of(c * half + i * 256, 256)
        return pl.ds(at, 256)

    def out_local(i, which):
        return pltpu.make_async_copy(
            staged.at[i, which], (og_ref, ou_ref)[which].at[0, out_rows(i), :], out_sem.at[i, which]
        )

    def out_remote(i, which):
        return pltpu.make_async_remote_copy(
            src_ref=staged.at[i, 2 + which],
            dst_ref=(og_ref, ou_ref)[which].at[0, out_rows(i), :],
            send_sem=out_send.at[i, which],
            recv_sem=out_recv.at[i, which],
            device_id=partner,
            device_id_type=pl.DeviceIdType.MESH,
        )

    all_rows = rows.shape[1] * rows.shape[2]

    @pl.loop(0, 8)
    def _(i):
        for stage in range(1, 5):
            @pl.when(i == stage)
            def _():
                reduce_stage(stage)
        def multiply(left):
            for q in range(4):
                staged[i, q] = lax.dot_general(
                    left, grads[:, q * units:(q + 1) * units], (((0,), (0,)), ((), ())),
                    preferred_element_type=F32,
                )

        @pl.when(i < 6)
        def _():
            at = pl.ds(pl.multiple_of(i % 3 * 256, 256), 256)
            multiply(rows[i // 3, :, :, at].reshape(all_rows, 256))

        @pl.when(i == 6)
        def _():
            for h in (0, 1):
                for n in range(4):
                    for dz in (2, 1, 3):
                        slots_out(h, n, dz).wait_recv()
                    slots_own(h, n).wait()

        @pl.when(i >= 6)
        def _():
            at = pl.ds(pl.multiple_of((i - 6) % 2 * 256, 256), 256)
            multiply(rows_f[:, :, :, :, :, at].reshape(all_rows, 256))

        for which in range(2):
            out_local(i, which).start()
            out_remote(i, which).start()

    terms_own.wait()
    for g in range(4):
        for dz in (2, 1, 3):
            terms_out(g, dz).wait_recv()
    make_totals()
    for h, o in around:
        back1(h, o).start()

    finish1(1)
    finish1(3)
    for h, s in both:
        reduce2(h, s, "o").start()
    relay1(0)
    for h, s in both:
        reduce2(h, s, "f").wait_recv()
        alpha, beta = along(h)
        add_into(h, block(h, shifted(alpha, SIGN[s], 4), beta), s, [(far2.at[h, s], 0)])
        reduce2(h, s, "w").start()
    for h in (0, 1):
        for o in (1, 2, 3):
            back1(h, o).wait_recv()
        base = along(h)[1] * 4

        @pl.loop(0, 4)
        def _(i):
            total = totals_f[h, base + i].astype(F32)
            for o in range(3):
                total = total + sums1_f[h, o, i].astype(F32)
            totals_f[h, base + i] = total.astype(BF16)

        for o in (2, 1, 3):
            back2(h, o).start()
    finish1(0)
    for h, s in both:
        reduce2(h, s, "o").wait_recv()
        reduce2(h, s, "w").wait_recv()
    for h in (0, 1):
        for p in (0, 1):
            base = p * part_rows
            add_into(h, here, p, [(near2.at[h, 0], base), (near2.at[h, 1], base)])

    for dz, dc in peers:
        bring(dz, dc).start()
    own_out.start()

    for h in (0, 1):
        for o in (1, 2, 3):
            back2(h, o).wait_recv()
        alpha, beta = along(h)
        total = totals_f[h, beta * 4 + alpha].astype(F32)
        for o in range(3):
            total = total + sums2_f[h, o].astype(F32)
        last_f[h] = total.astype(BF16)
    last_out().start()
    last_own.start()
    last_own.wait()
    last_out().wait_recv()
    own_out.wait()
    for dz, dc in peers:
        bring(dz, dc).wait_recv()
    for dz, dc in peers:
        spread(dz, dc).wait_send()
        bring(dz, dc).wait_send()
    for which in range(2):
        weight_out(which).wait_send()
    grads_out().wait_send()
    block_out().wait_send()
    last_out().wait_send()
    for h, o in around:
        plane1(h, o).wait_send()
        plane2(h, o).wait_send()
        back1(h, o).wait_send()
        back2(h, o).wait_send()
    for h in (0, 1):
        for n in range(4):
            for dz in (2, 1, 3):
                slots_out(h, n, dz).wait_send()
    for g in range(4):
        for dz in (2, 1, 3):
            terms_out(g, dz).wait_send()
    for h, s in both:
        for t in ("f", "o", "w"):
            gather1(h, s, t).wait_send()
            reduce2(h, s, t).wait_send()
            for k in range(4):
                gather2(h, s, k, t).wait_send()
                reduce1(h, s, k, t).wait_send()

    @pl.loop(0, 8)
    def _(i):
        for which in range(2):
            out_local(i, which).wait()
            out_remote(i, which).wait()


MESSAGES = 7 + 7 + 2 + 1 + 12 + 48 + 48 + 12 + 1 + 1 + 4 * 6 + 24 + 12


def on_device(tokens, expert_ids, weight_gate, weight_up, gate_pre, up_pre, hidden_grad):
    count, width = tokens.shape
    slots, units = gate_pre.shape[1:]
    wide_f = width // 8
    quarter = (width // 2 - wide_f) // 2
    lines = slots // 16
    vmem = pl.BlockSpec(memory_space=pltpu.VMEM)
    anywhere = pl.BlockSpec(memory_space=pl.ANY)
    dma = pltpu.SemaphoreType.DMA
    ids_t = expert_ids.T
    returned, summed, gate_out, up_out = pl.pallas_call(
        kernel,
        out_shape=(
            pltpu.VMEM((2, 2, 64, quarter), BF16),
            pltpu.VMEM((2, 32, wide_f), BF16),
            pltpu.VMEM((1, width, units), F32),
            pltpu.VMEM((1, width, units), F32),
        ),
        in_specs=[vmem] * 2 + [anywhere] * 5,
        out_specs=(anywhere,) * 4,
        scratch_shapes=[
            pltpu.VMEM((2, 16, lines, quarter), BF16),
            pltpu.VMEM((4, 4, 2, 4, 16, wide_f), BF16),
            pltpu.VMEM((slots, 4 * units), BF16),
            pltpu.VMEM((width // 2, 4 * units), BF16),
            pltpu.VMEM((2, 16, lines, quarter), BF16),
            pltpu.VMEM((4, 4, 2, 4, 16, wide_f), BF16),
            pltpu.VMEM((2, 2, 4, lines, quarter), BF16),
            pltpu.VMEM((2, 2, 4, lines // 2, quarter), BF16),
            pltpu.VMEM((2, 2, lines, quarter), BF16),
            pltpu.VMEM((2, 2, lines // 2, quarter), BF16),
            pltpu.VMEM((8, 4, 256, units), F32),
            pltpu.VMEM((3, slots, units), BF16),
            pltpu.VMEM((2, 2, 64, quarter), BF16),
            pltpu.VMEM((2, 32, wide_f), BF16),
            pltpu.VMEM((2, 16, 32, wide_f), BF16),
            pltpu.VMEM((2, 4, 4, 64, wide_f), BF16),
            pltpu.VMEM((4, 4, 4, 2, 16, wide_f), BF16),
            pltpu.VMEM((2, 16, 32, wide_f), BF16),
            pltpu.VMEM((2, 3, 4, 32, wide_f), BF16),
            pltpu.VMEM((2, 3, 32, wide_f), BF16),
            pltpu.VMEM((2, 32, wide_f), BF16),
            dma((MESSAGES,)),
            dma((MESSAGES,)),
            dma((18,)),
            dma((8, 2)),
            dma((8, 2)),
            dma((8, 2)),
        ],
        compiler_params=pltpu.CompilerParams(
            collective_id=0, has_side_effects=True, vmem_limit_bytes=51 * 1024 * 1024
        ),
    )(ids_t, tokens, weight_gate, weight_up, gate_pre, up_pre, hidden_grad)
    return pl.pallas_call(
        finish,
        out_shape=(
            jax.ShapeDtypeStruct((count, width), BF16),
            jax.ShapeDtypeStruct((1, width, units), F32),
            jax.ShapeDtypeStruct((1, width, units), F32),
        ),
        in_specs=[vmem, vmem, vmem, anywhere, anywhere],
        out_specs=(vmem, anywhere, anywhere),
        scratch_shapes=[dma((8,))],
        compiler_params=pltpu.CompilerParams(vmem_limit_bytes=8 * 1024 * 1024),
    )(ids_t, returned, summed, gate_out, up_out)


def solution(mesh):
    torus = Mesh(
        mesh.devices.reshape(mesh.shape["expert"], 4, 4, 2),
        ("expert", "shard_0", "shard_1", "shard_2"),
    )
    split = P("expert", None, SHARD)
    placed = (P(EXPERT_SHARD, None), P(EXPERT_SHARD, None), split, split, split, split, split)
    return jax.shard_map(
        on_device,
        mesh=torus,
        in_specs=placed,
        out_specs=(P(EXPERT_SHARD, None), split, split),
        check_vma=False,
    )
```

```python
import functools

import jax
import jax.numpy as jnp
from jax import lax
from jax.experimental import pallas as pl
from jax.experimental.pallas import tpu as pltpu
from jax.sharding import Mesh
from jax.sharding import PartitionSpec as P

SHARD = ("shard_0", "shard_1", "shard_2")
EXPERT_SHARD = ("expert", "shard_0", "shard_1", "shard_2")
SIGN = (1, -1)
F32 = jnp.float32
BF16 = jnp.bfloat16


def shifted(value, by, size):
    return lax.rem(value + by % size, size)


def picked(first_ids, second_ids, cap):
    tokens = first_ids.shape[1]
    line = lax.broadcasted_iota(jnp.int32, (4 * cap, tokens), 0)
    expert = (line // cap).astype(F32)
    named = (first_ids == expert) | (second_ids == expert)
    before = (
        lax.broadcasted_iota(jnp.int32, (tokens, tokens), 0)
        < lax.broadcasted_iota(jnp.int32, (tokens, tokens), 1)
    )
    slot = jnp.dot(
        named.astype(F32).astype(BF16), before.astype(F32).astype(BF16), preferred_element_type=F32
    )
    return jnp.where(named & (slot == (line % cap).astype(F32)), 1.0, 0.0).astype(BF16)


def finish(ids_t_ref, returned, summed, og_in, ou_in, tg_ref, og_ref, ou_ref, sems):
    width = og_in.shape[1] // 4

    def put(i):
        which, q = i // 4, i % 4
        at = pl.ds(q * width, width)
        return pltpu.make_async_copy(
            (og_in, ou_in)[which].at[0, at, :], (og_ref, ou_ref)[which].at[0, at, :], sems.at[i]
        )

    for i in range(8):
        put(i).start()
    ids = ids_t_ref[...].astype(F32)
    pick_t = picked(ids[0:1, :], ids[1:2, :], 16)
    tokens = tg_ref.shape[0]
    half = tg_ref.shape[1] // 2
    quarter = returned.shape[3]
    for core in range(2):
        for h in range(2):
            at = core * half + h * quarter
            tg_ref[:, at:at + quarter] = lax.dot_general(
                pick_t, returned[core, h], (((0,), (0,)), ((), ())), preferred_element_type=F32
            ).astype(BF16)
        at = core * half + 2 * quarter
        tg_ref[:, at:(core + 1) * half] = summed[core]
    for i in range(8):
        put(i).wait()


def kernel(
    ids_t_ref, tok_ref, wg_ref, wu_ref, gate_ref, up_ref, hid_ref,
    returned, summed, og_ref, ou_ref,
    rows, rows_f, grads, weights, terms, terms_f, near1, far1, near2, far2, staged, pre, outgoing,
    block_f, plane_f, slots_f, crossed_f, totals_f, sums1_f, sums2_f, last_f,
    send_sem, recv_sem, local_sem, out_sem, out_send, out_recv,
):
    z = lax.axis_index("expert")
    y = lax.axis_index("shard_0")
    x = lax.axis_index("shard_1")
    c = lax.axis_index("shard_2")
    other = 1 - c
    here = y * 4 + x
    half = tok_ref.shape[1] // 2
    quarter = rows.shape[3]
    wide_f = rows_f.shape[5]
    units = gate_ref.shape[2]
    tokens = tok_ref.shape[0]
    cap = 16
    part_rows = rows.shape[2] // 2

    numbers = {}

    def number(key):
        return numbers.setdefault(key, len(numbers))

    def remote(key, src, dst, device):
        i = number(key)
        return pltpu.make_async_remote_copy(
            src_ref=src,
            dst_ref=dst,
            send_sem=send_sem.at[i],
            recv_sem=recv_sem.at[i],
            device_id=device,
            device_id_type=pl.DeviceIdType.MESH,
        )

    def along(h):
        return (x, y) if h == 0 else (y, x)

    def block(h, alpha, beta):
        return beta * 4 + alpha if h == 0 else alpha * 4 + beta

    def first(h, s):
        return {"shard_1": shifted(x, SIGN[s], 4)} if h == 0 else {"shard_0": shifted(y, SIGN[s], 4)}

    def second(h, s):
        return first(1 - h, s)

    def part(p):
        return pl.ds(p * part_rows, part_rows)

    def gather1(h, s, t, arriving=False):
        alpha, beta = along(h)
        back = (1 if t == "w" else 0) + (1 if arriving else 0)
        p = 1 - s if t == "o" else s
        ref = rows.at[h, block(h, shifted(alpha, -SIGN[s] * back, 4), beta), part(p)]
        return remote(("a1", h, s, t), ref, ref, first(h, s))

    def gather2(h, s, k, t, arriving=False):
        alpha, beta = along(h)
        back = (1 if t == "w" else 0) + (1 if arriving else 0)
        p = 1 - s if t == "o" else s
        ref = rows.at[
            h, block(h, shifted(alpha, k, 4), shifted(beta, -SIGN[s] * back, 4)), part(p)
        ]
        return remote(("a2", h, s, k, t), ref, ref, second(h, s))

    def reduce1(h, s, k, t):
        alpha, beta = along(h)
        a = shifted(alpha, k, 4)
        if t == "f":
            src = terms.at[h, block(h, a, shifted(beta, 2, 4)), part(s)]
            dst = far1.at[h, s, k]
        else:
            p = 1 - s if t == "o" else s
            src = terms.at[h, block(h, a, shifted(beta, SIGN[s], 4)), part(p)]
            dst = near1.at[h, s, k, part(p)]
        return remote(("r1", h, s, k, t), src, dst, second(h, s))

    def reduce2(h, s, t):
        alpha, beta = along(h)
        if t == "f":
            src = terms.at[h, block(h, shifted(alpha, 2, 4), beta), part(s)]
            dst = far2.at[h, s]
        else:
            p = 1 - s if t == "o" else s
            src = terms.at[h, block(h, shifted(alpha, SIGN[s], 4), beta), part(p)]
            dst = near2.at[h, s, part(p)]
        return remote(("r2", h, s, t), src, dst, first(h, s))

    def slots_of(device, core):
        return pl.ds(pl.multiple_of(core * 64 + device * cap, cap), cap)

    def spread(dz, dc):
        e = shifted(z, dz, 4)
        core = shifted(c, dc, 2)
        return remote(
            ("zi", dz, dc),
            outgoing.at[core, :, pl.ds(pl.multiple_of(e * cap, cap), cap), :],
            rows.at[:, here, slots_of(z, c), :],
            {"expert": e, "shard_2": core},
        )

    def bring(dz, dc):
        j = shifted(z, dz, 4)
        core = shifted(c, dc, 2)
        return remote(
            ("zo", dz, dc),
            terms.at[:, here, slots_of(j, core), :],
            returned.at[c, :, pl.ds(pl.multiple_of(z * cap, cap), cap), :],
            {"expert": j, "shard_2": core},
        )

    partner = {"shard_2": other}

    def aside1(h, o):
        return {"shard_1": shifted(x, o, 4)} if h == 0 else {"shard_0": shifted(y, o, 4)}

    def aside2(h, o):
        return aside1(1 - h, o)

    def block_out():
        return remote(
            ("fb",), block_f.at[other], plane_f.at[c, here * (1 - c) + (x * 4 + y) * c], partner
        )

    block_own = pltpu.make_async_copy(
        block_f.at[c], plane_f.at[c, here * (1 - c) + (x * 4 + y) * c], local_sem.at[7]
    )

    def plane1(h, o):
        alpha, beta = along(h)
        ref = plane_f.at[h, beta * 4 + alpha]
        return remote(("f1", h, o), ref, ref, aside1(h, o))

    def plane2(h, o):
        alpha, beta = along(h)
        ref = plane_f.at[h, pl.ds(beta * 4, 4)]
        return remote(("f2", h, o), ref, ref, aside2(h, o))

    def group_rows(h, at, j):
        return rows_f.at[at, :, 0, j] if h == 0 else rows_f.at[:, at, 1, j]

    TURN = (0, 1, 3, 2)

    def slots_out(h, n, dz):
        e = shifted(z, dz, 4)
        at = shifted(along(h)[1], TURN[n], 4)
        return remote(
            ("fz", h, n, dz),
            slots_f.at[h, n, :, pl.ds(pl.multiple_of(e * cap, cap), cap), :],
            group_rows(h, at, z),
            {"expert": e},
        )

    def slots_own(h, n):
        at = shifted(along(h)[1], TURN[n], 4)
        return pltpu.make_async_copy(
            slots_f.at[h, n, :, pl.ds(pl.multiple_of(z * cap, cap), cap), :],
            group_rows(h, at, z),
            local_sem.at[8 + h * 4 + n],
        )

    def picked_of(h, at):
        ids = plane_f[h, at, tokens:tokens + 8, 0:128].astype(F32)
        lines = plane_f.shape[2]
        return picked(ids[0:1, 0:lines], ids[1:2, 0:lines], cap)

    def make_slots(h, n):
        at = shifted(along(h)[1], TURN[n], 4)

        @pl.loop(0, 4)
        def _(i):
            slots_f[h, n, i] = jnp.dot(
                picked_of(h, at * 4 + i), plane_f[h, at * 4 + i], preferred_element_type=F32
            ).astype(BF16)

        for dz in (2, 1, 3):
            slots_out(h, n, dz).start()
        slots_own(h, n).start()

    def terms_out(g, dz):
        j = shifted(z, dz, 4)
        return remote(
            ("ft", g, dz), terms_f.at[g, :, :, j], crossed_f.at[z, g], {"expert": j}
        )

    terms_own = pltpu.make_async_copy(terms_f.at[:, :, :, z], crossed_f.at[z], local_sem.at[16])

    def make_totals():
        for h in (0, 1):
            @pl.loop(0, 16)
            def _(i):
                one, two = i // 4, i % 4
                held = crossed_f[:, one, two, 0] if h == 0 else crossed_f[:, two, one, 1]
                totals_f[h, i] = lax.dot_general(
                    picked_of(h, i)[:, 0:tokens], held.reshape(4 * cap, wide_f),
                    (((0,), (0,)), ((), ())), preferred_element_type=F32,
                ).astype(BF16)

    def back1(h, o):
        alpha, beta = along(h)
        return remote(
            ("b1", h, o), totals_f.at[h, pl.ds(shifted(beta, o, 4) * 4, 4)],
            sums1_f.at[h, o - 1], aside2(h, o),
        )

    def back2(h, o):
        alpha, beta = along(h)
        return remote(
            ("b2", h, o), totals_f.at[h, beta * 4 + shifted(alpha, o, 4)],
            sums2_f.at[h, o - 1], aside1(h, o),
        )

    def last_out():
        return remote(("fl",), last_f.at[other], summed.at[c], partner)

    last_own = pltpu.make_async_copy(last_f.at[c], summed.at[c], local_sem.at[17])
    around = [(h, o) for o in (2, 1, 3) for h in (0, 1)]

    def weight_out(which):
        ref = (wg_ref, wu_ref)[which]
        return remote(
            ("w", which),
            ref.at[0, pl.ds(pl.multiple_of(other * half, half), half), :],
            weights.at[:, pl.ds(2 * units + which * units, units)],
            partner,
        )

    def weight_in(which):
        ref = (wg_ref, wu_ref)[which]
        return pltpu.make_async_copy(
            ref.at[0, pl.ds(pl.multiple_of(c * half, half), half), :],
            weights.at[:, pl.ds(which * units, units)],
            local_sem.at[which],
        )

    def pre_in(which):
        ref = (gate_ref, up_ref, hid_ref)[which]
        return pltpu.make_async_copy(ref.at[0], pre.at[which], local_sem.at[2 + which])

    def grads_out():
        return remote(
            ("g",), grads.at[:, pl.ds(0, 2 * units)], grads.at[:, pl.ds(2 * units, 2 * units)], partner
        )

    own_in = pltpu.make_async_copy(
        outgoing.at[c, :, pl.ds(pl.multiple_of(z * cap, cap), cap), :],
        rows.at[:, here, slots_of(z, c), :],
        local_sem.at[5],
    )

    own_out = pltpu.make_async_copy(
        terms.at[:, here, slots_of(z, c), :],
        returned.at[c, :, pl.ds(pl.multiple_of(z * cap, cap), cap), :],
        local_sem.at[6],
    )

    peers = [(dz, dc) for dz in (2, 1, 3, 0) for dc in (0, 1) if (dz, dc) != (0, 0)]
    both = [(h, s) for h in (0, 1) for s in (0, 1)]

    for which in range(3):
        pre_in(which).start()
    for which in range(2):
        weight_in(which).start()
    barrier = pltpu.get_barrier_semaphore()
    for dz, dc in peers:
        pl.semaphore_signal(
            barrier, inc=1,
            device_id={"expert": shifted(z, dz, 4), "shard_2": shifted(c, dc, 2)},
            device_id_type=pl.DeviceIdType.MESH,
        )
    for h, s in both:
        pl.semaphore_signal(
            barrier, inc=1, device_id=first(h, s), device_id_type=pl.DeviceIdType.MESH
        )
    for h in (0, 1):
        pl.semaphore_signal(
            barrier, inc=1, device_id=aside1(h, 2), device_id_type=pl.DeviceIdType.MESH
        )

    ids = ids_t_ref[...].astype(F32)
    pick_t = picked(ids[0:1, :], ids[1:2, :], cap)
    for core in range(2):
        at = core * half + 2 * quarter
        block_f[core, 0:tokens, :] = tok_ref[:, at:at + wide_f]
        block_f[core, tokens:, :] = jnp.full((block_f.shape[1] - tokens, wide_f), 9.0, BF16)
        block_f[core, tokens:tokens + 2, 0:tokens] = ids.astype(BF16)
    for core in range(2):
        for h in range(2):
            at = core * half + h * quarter
            outgoing[core, h] = jnp.dot(
                pick_t, tok_ref[:, at:at + quarter], preferred_element_type=F32
            ).astype(BF16)

    pl.semaphore_wait(barrier, len(peers) + len(both) + 2)
    block_out().start()
    block_own.start()
    for dz, dc in peers:
        spread(dz, dc).start()
    own_in.start()
    block_own.wait()
    block_out().wait_recv()
    for h, o in around:
        plane1(h, o).start()

    for which in range(2):
        weight_out(which).start()

    for which in range(3):
        pre_in(which).wait()

    pieces = pre.shape[1] // 64

    def make_grads(i):
        at = pl.ds(pl.multiple_of(i * 64, 64), 64)
        a = pre[0, at, :].astype(F32)
        b = pre[1, at, :].astype(F32)
        g = pre[2, at, :].astype(F32)
        sig = 1.0 / (1.0 + jnp.exp(-a))
        gs = g * sig
        grads[at, 0:units] = (gs * b * (1.0 + a * (1.0 - sig))).astype(BF16)
        grads[at, units:2 * units] = (gs * a).astype(BF16)

    pl.loop(0, pieces // 2)(make_grads)
    for h, o in around:
        plane1(h, o).wait_recv()
    for h, o in around:
        plane2(h, o).start()
    pl.loop(pieces // 2, pieces)(make_grads)
    grads_out().start()

    own_in.wait()
    for dz, dc in peers:
        spread(dz, dc).wait_recv()
    for t in ("f", "o"):
        for h, s in both:
            gather1(h, s, t).start()
    for t in ("f", "o"):
        for h, s in both:
            gather2(h, s, 0, t).start()

    def send_part(h, k, p):
        for s in ((0, 1) if p == 0 else (1, 0)):
            gather2(h, s, k, "f" if s == p else "o").start()

    def group_stage(n):
        for h in (0, 1):
            if n:
                plane2(h, (None, 3, 1, 2)[n]).wait_recv()
            make_slots(h, n)

    def gather_stage(i):
        if i == 0:
            group_stage(0)
        if i == 1:
            for h, s in both:
                gather1(h, s, "f", True).wait_recv()
                gather1(h, s, "w").start()
            for h in (0, 1):
                send_part(h, 3, 0)
                send_part(h, 1, 1)
        if i == 2:
            for h, s in both:
                gather1(h, s, "o", True).wait_recv()
            for h in (0, 1):
                send_part(h, 3, 1)
                send_part(h, 1, 0)
            for g in range(4):
                for dz in (2, 1, 3):
                    terms_out(g, dz).start()
            terms_own.start()
        if i == 3:
            for h, s in both:
                gather2(h, s, 0, "f", True).wait_recv()
                gather2(h, s, 0, "w").start()
            group_stage(1)
        if i == 4:
            for h, s in both:
                gather1(h, s, "w", True).wait_recv()
            for h in (0, 1):
                gather2(h, 0, 2, "f").start()
                gather2(h, 1, 2, "f").start()
                gather2(h, 0, 2, "o").start()
                gather2(h, 1, 2, "o").start()
            group_stage(2)
        if i == 5:
            for h in (0, 1):
                for s, k in ((0, 3), (1, 1)):
                    gather2(h, s, k, "f", True).wait_recv()
                    gather2(h, s, k, "w").start()
            group_stage(3)
        if i == 6:
            for h in (0, 1):
                for s, k in ((0, 1), (1, 3)):
                    gather2(h, s, k, "f", True).wait_recv()
                    gather2(h, s, k, "w").start()

    for which in range(2):
        weight_in(which).wait()
        weight_out(which).wait_recv()
    grads_out().wait_recv()

    group = 4 * rows.shape[2]

    @pl.loop(0, 8)
    def _(i):
        for stage in range(7):
            @pl.when(i == stage)
            def _():
                gather_stage(stage)
        tile = (i + 6) % 8

        @pl.loop(0, 4)
        def _(g):
            left = grads[pl.ds(pl.multiple_of(g * group, group), group), :]
            right = weights[pl.ds(pl.multiple_of(tile * 256, 256), 256), :]
            out = lax.dot_general(
                left, right, (((1,), (1,)), ((), ())), preferred_element_type=F32
            ).astype(BF16)

            @pl.when(tile < 6)
            def _():
                terms[
                    tile // 3, pl.ds(g * 4, 4), :, pl.ds(pl.multiple_of(tile % 3 * 256, 256), 256)
                ] = out.reshape(4, rows.shape[2], 256)

            for m in range(2):
                @pl.when(tile == 6 + m)
                def _():
                    terms_f[g, :, :, :, :, m * 256:(m + 1) * 256] = out.reshape(4, 2, 4, cap, 256)

    for h, s in both:
        gather2(h, s, 2, "f", True).wait_recv()
        gather2(h, s, 2, "w").start()

    for k, t in ((2, "f"), (1, "f"), (2, "o"), (3, "f")):
        for h, s in both:
            reduce1(h, s, k, t).start()

    for h, s in both:
        for k in (0, 1, 3, 2):
            gather2(h, s, k, "o", True).wait_recv()
            gather2(h, s, k, "w", True).wait_recv()

    def add_into(h, at, p, sources):
        @pl.loop(0, part_rows // 16)
        def _(i):
            lines = pl.ds(pl.multiple_of(p * part_rows + i * 16, 16), 16)
            total = terms[h, at, lines, :].astype(F32)
            for ref, base in sources:
                total = total + ref[
                    pl.ds(pl.multiple_of(base + i * 16, 16), 16), :
                ].astype(F32)
            terms[h, at, lines, :] = total.astype(BF16)

    def relay1(k):
        for h, s in both:
            reduce1(h, s, k, "f").wait_recv()
            alpha, beta = along(h)
            add_into(
                h, block(h, shifted(alpha, k, 4), shifted(beta, SIGN[s], 4)), s,
                [(far1.at[h, s, k], 0)],
            )
            reduce1(h, s, k, "w").start()

    def finish1(k):
        for h in (0, 1):
            for s in (0, 1):
                reduce1(h, s, k, "o").wait_recv()
                reduce1(h, s, k, "w").wait_recv()
            alpha, beta = along(h)
            for p in (0, 1):
                base = p * part_rows
                add_into(
                    h, block(h, shifted(alpha, k, 4), beta), p,
                    [(near1.at[h, 0, k], base), (near1.at[h, 1, k], base)],
                )

    def send1(k, t):
        for h, s in both:
            reduce1(h, s, k, t).start()

    def reduce_stage(i):
        if i == 1:
            relay1(2)
            send1(1, "o")
        if i == 2:
            relay1(1)
            send1(3, "o")
        if i == 3:
            relay1(3)
            send1(0, "f")
        if i == 4:
            finish1(2)
            for h, s in both:
                reduce2(h, s, "f").start()
            send1(0, "o")
        if i == 5:
            terms_own.wait()
            for g in range(4):
                for dz in (2, 1, 3):
                    terms_out(g, dz).wait_recv()
            make_totals()
        if i == 6:
            finish1(1)
            finish1(3)
            for h, s in both:
                reduce2(h, s, "o").start()
            relay1(0)
        if i == 7:
            for h, s in both:
                reduce2(h, s, "f").wait_recv()
                alpha, beta = along(h)
                add_into(h, block(h, shifted(alpha, SIGN[s], 4), beta), s, [(far2.at[h, s], 0)])
                reduce2(h, s, "w").start()
            for h, o in around:
                back1(h, o).start()

    def out_rows(i):
        at = pl.multiple_of(c * half + i * 256, 256)
        return pl.ds(at, 256)

    def out_local(i, which):
        return pltpu.make_async_copy(
            staged.at[i, which], (og_ref, ou_ref)[which].at[0, out_rows(i), :], out_sem.at[i, which]
        )

    def out_remote(i, which):
        return pltpu.make_async_remote_copy(
            src_ref=staged.at[i, 2 + which],
            dst_ref=(og_ref, ou_ref)[which].at[0, out_rows(i), :],
            send_sem=out_send.at[i, which],
            recv_sem=out_recv.at[i, which],
            device_id=partner,
            device_id_type=pl.DeviceIdType.MESH,
        )

    all_rows = rows.shape[1] * rows.shape[2]

    @pl.loop(0, 8)
    def _(i):
        for stage in range(1, 8):
            @pl.when(i == stage)
            def _():
                reduce_stage(stage)
        def multiply(left):
            for q in range(4):
                staged[i, q] = lax.dot_general(
                    left, grads[:, q * units:(q + 1) * units], (((0,), (0,)), ((), ())),
                    preferred_element_type=F32,
                )

        @pl.when(i < 6)
        def _():
            at = pl.ds(pl.multiple_of(i % 3 * 256, 256), 256)
            multiply(rows[i // 3, :, :, at].reshape(all_rows, 256))

        @pl.when(i == 6)
        def _():
            for h in (0, 1):
                for n in range(4):
                    for dz in (2, 1, 3):
                        slots_out(h, n, dz).wait_recv()
                    slots_own(h, n).wait()

        @pl.when(i >= 6)
        def _():
            at = pl.ds(pl.multiple_of((i - 6) % 2 * 256, 256), 256)
            multiply(rows_f[:, :, :, :, :, at].reshape(all_rows, 256))

        for which in range(2):
            out_local(i, which).start()
            out_remote(i, which).start()

    finish1(0)
    for h, s in both:
        reduce2(h, s, "o").wait_recv()
        reduce2(h, s, "w").wait_recv()
    for h in (0, 1):
        for p in (0, 1):
            base = p * part_rows
            add_into(h, here, p, [(near2.at[h, 0], base), (near2.at[h, 1], base)])

    for dz, dc in peers:
        bring(dz, dc).start()
    own_out.start()

    for h in (0, 1):
        for o in (1, 2, 3):
            back1(h, o).wait_recv()
        base = along(h)[1] * 4

        @pl.loop(0, 4)
        def _(i):
            total = totals_f[h, base + i].astype(F32)
            for o in range(3):
                total = total + sums1_f[h, o, i].astype(F32)
            totals_f[h, base + i] = total.astype(BF16)

        for o in (2, 1, 3):
            back2(h, o).start()


    for h in (0, 1):
        for o in (1, 2, 3):
            back2(h, o).wait_recv()
        alpha, beta = along(h)
        total = totals_f[h, beta * 4 + alpha].astype(F32)
        for o in range(3):
            total = total + sums2_f[h, o].astype(F32)
        last_f[h] = total.astype(BF16)
    last_out().start()
    last_own.start()
    last_own.wait()
    last_out().wait_recv()
    own_out.wait()
    for dz, dc in peers:
        bring(dz, dc).wait_recv()
    for dz, dc in peers:
        spread(dz, dc).wait_send()
        bring(dz, dc).wait_send()
    for which in range(2):
        weight_out(which).wait_send()
    grads_out().wait_send()
    block_out().wait_send()
    last_out().wait_send()
    for h, o in around:
        plane1(h, o).wait_send()
        plane2(h, o).wait_send()
        back1(h, o).wait_send()
        back2(h, o).wait_send()
    for h in (0, 1):
        for n in range(4):
            for dz in (2, 1, 3):
                slots_out(h, n, dz).wait_send()
    for g in range(4):
        for dz in (2, 1, 3):
            terms_out(g, dz).wait_send()
    for h, s in both:
        for t in ("f", "o", "w"):
            gather1(h, s, t).wait_send()
            reduce2(h, s, t).wait_send()
            for k in range(4):
                gather2(h, s, k, t).wait_send()
                reduce1(h, s, k, t).wait_send()

    @pl.loop(0, 8)
    def _(i):
        for which in range(2):
            out_local(i, which).wait()
            out_remote(i, which).wait()


MESSAGES = 7 + 7 + 2 + 1 + 12 + 48 + 48 + 12 + 1 + 1 + 4 * 6 + 24 + 12


def on_device(tokens, expert_ids, weight_gate, weight_up, gate_pre, up_pre, hidden_grad):
    count, width = tokens.shape
    slots, units = gate_pre.shape[1:]
    wide_f = width // 8
    quarter = (width // 2 - wide_f) // 2
    lines = slots // 16
    vmem = pl.BlockSpec(memory_space=pltpu.VMEM)
    anywhere = pl.BlockSpec(memory_space=pl.ANY)
    dma = pltpu.SemaphoreType.DMA
    ids_t = expert_ids.T
    returned, summed, gate_out, up_out = pl.pallas_call(
        kernel,
        out_shape=(
            pltpu.VMEM((2, 2, 64, quarter), BF16),
            pltpu.VMEM((2, count, wide_f), BF16),
            pltpu.VMEM((1, width, units), F32),
            pltpu.VMEM((1, width, units), F32),
        ),
        in_specs=[vmem] * 2 + [anywhere] * 5,
        out_specs=(anywhere,) * 4,
        scratch_shapes=[
            pltpu.VMEM((2, 16, lines, quarter), BF16),
            pltpu.VMEM((4, 4, 2, 4, 16, wide_f), BF16),
            pltpu.VMEM((slots, 4 * units), BF16),
            pltpu.VMEM((width // 2, 4 * units), BF16),
            pltpu.VMEM((2, 16, lines, quarter), BF16),
            pltpu.VMEM((4, 4, 2, 4, 16, wide_f), BF16),
            pltpu.VMEM((2, 2, 4, lines, quarter), BF16),
            pltpu.VMEM((2, 2, 4, lines // 2, quarter), BF16),
            pltpu.VMEM((2, 2, lines, quarter), BF16),
            pltpu.VMEM((2, 2, lines // 2, quarter), BF16),
            pltpu.VMEM((8, 4, 256, units), F32),
            pltpu.VMEM((3, slots, units), BF16),
            pltpu.VMEM((2, 2, 64, quarter), BF16),
            pltpu.VMEM((2, 32, wide_f), BF16),
            pltpu.VMEM((2, 16, 32, wide_f), BF16),
            pltpu.VMEM((2, 4, 4, 64, wide_f), BF16),
            pltpu.VMEM((4, 4, 4, 2, 16, wide_f), BF16),
            pltpu.VMEM((2, 16, count, wide_f), BF16),
            pltpu.VMEM((2, 3, 4, count, wide_f), BF16),
            pltpu.VMEM((2, 3, count, wide_f), BF16),
            pltpu.VMEM((2, count, wide_f), BF16),
            dma((MESSAGES,)),
            dma((MESSAGES,)),
            dma((18,)),
            dma((8, 2)),
            dma((8, 2)),
            dma((8, 2)),
        ],
        compiler_params=pltpu.CompilerParams(
            collective_id=0, has_side_effects=True, vmem_limit_bytes=51 * 1024 * 1024
        ),
    )(ids_t, tokens, weight_gate, weight_up, gate_pre, up_pre, hidden_grad)
    return pl.pallas_call(
        finish,
        out_shape=(
            jax.ShapeDtypeStruct((count, width), BF16),
            jax.ShapeDtypeStruct((1, width, units), F32),
            jax.ShapeDtypeStruct((1, width, units), F32),
        ),
        in_specs=[vmem, vmem, vmem, anywhere, anywhere],
        out_specs=(vmem, anywhere, anywhere),
        scratch_shapes=[dma((8,))],
        compiler_params=pltpu.CompilerParams(vmem_limit_bytes=8 * 1024 * 1024),
    )(ids_t, returned, summed, gate_out, up_out)


def solution(mesh):
    torus = Mesh(
        mesh.devices.reshape(mesh.shape["expert"], 4, 4, 2),
        ("expert", "shard_0", "shard_1", "shard_2"),
    )
    split = P("expert", None, SHARD)
    placed = (P(EXPERT_SHARD, None), P(EXPERT_SHARD, None), split, split, split, split, split)
    return jax.shard_map(
        on_device,
        mesh=torus,
        in_specs=placed,
        out_specs=(P(EXPERT_SHARD, None), split, split),
        check_vma=False,
    )
```

```python
import functools

import jax
import jax.numpy as jnp
from jax import lax
from jax.experimental import pallas as pl
from jax.experimental.pallas import tpu as pltpu
from jax.sharding import Mesh
from jax.sharding import PartitionSpec as P

SHARD = ("shard_0", "shard_1", "shard_2")
EXPERT_SHARD = ("expert", "shard_0", "shard_1", "shard_2")
SIGN = (1, -1)
F32 = jnp.float32
BF16 = jnp.bfloat16


def shifted(value, by, size):
    return lax.rem(value + by % size, size)


def picked(first_ids, second_ids, cap):
    tokens = first_ids.shape[1]
    line = lax.broadcasted_iota(jnp.int32, (4 * cap, tokens), 0)
    expert = (line // cap).astype(F32)
    named = (first_ids == expert) | (second_ids == expert)
    before = (
        lax.broadcasted_iota(jnp.int32, (tokens, tokens), 0)
        < lax.broadcasted_iota(jnp.int32, (tokens, tokens), 1)
    )
    slot = jnp.dot(
        named.astype(F32).astype(BF16), before.astype(F32).astype(BF16), preferred_element_type=F32
    )
    return jnp.where(named & (slot == (line % cap).astype(F32)), 1.0, 0.0).astype(BF16)


def finish(ids_t_ref, returned, summed, og_in, ou_in, tg_out, og_ref, ou_ref, tg_ref, sems):
    width = og_in.shape[1] // 4

    def put(i):
        which, q = i // 4, i % 4
        at = pl.ds(q * width, width)
        return pltpu.make_async_copy(
            (og_in, ou_in)[which].at[0, at, :], (og_ref, ou_ref)[which].at[0, at, :], sems.at[i]
        )

    for i in range(8):
        put(i).start()
    ids = ids_t_ref[...].astype(F32)
    pick_t = picked(ids[0:1, :], ids[1:2, :], 16)
    tokens = tg_ref.shape[0]
    half = tg_ref.shape[1] // 2
    quarter = returned.shape[3]
    for core in range(2):
        for h in range(2):
            at = core * half + h * quarter
            tg_ref[:, at:at + quarter] = lax.dot_general(
                pick_t, returned[core, h], (((0,), (0,)), ((), ())), preferred_element_type=F32
            ).astype(BF16)
        at = core * half + 2 * quarter
        tg_ref[:, at:(core + 1) * half] = summed[core]
    tg_copy = pltpu.make_async_copy(tg_ref, tg_out, sems.at[8])
    tg_copy.start()
    for i in range(8):
        put(i).wait()
    tg_copy.wait()


class Together:
    def __init__(self, *copies):
        self.copies = copies

    def start(self):
        for copy in self.copies:
            copy.start()

    def wait_recv(self):
        for copy in self.copies:
            copy.wait_recv()

    def wait_send(self):
        for copy in self.copies:
            copy.wait_send()


def kernel(
    ids_any, tok_any, wg_ref, wu_ref, gate_ref, up_ref, hid_ref,
    returned, summed, og_ref, ou_ref,
    rows, rows_f, grads, weights, terms, terms_f, near1, far1, near2, far2, staged, pre, outgoing,
    block_f, plane_f, slots_f, crossed_f, totals_f, sums1_f, sums2_f, last_f,
    ids_t_ref, tok_ref, block_ids, plane_ids,
    send_sem, recv_sem, local_sem, out_sem, out_send, out_recv,
):
    z = lax.axis_index("expert")
    y = lax.axis_index("shard_0")
    x = lax.axis_index("shard_1")
    c = lax.axis_index("shard_2")
    other = 1 - c
    here = y * 4 + x
    half = tok_ref.shape[1] // 2
    quarter = rows.shape[3]
    wide_f = rows_f.shape[5]
    units = gate_ref.shape[2]
    tokens = tok_ref.shape[0]
    cap = 16
    part_rows = rows.shape[2] // 2

    numbers = {}

    def number(key):
        return numbers.setdefault(key, len(numbers))

    def remote(key, src, dst, device):
        i = number(key)
        return pltpu.make_async_remote_copy(
            src_ref=src,
            dst_ref=dst,
            send_sem=send_sem.at[i],
            recv_sem=recv_sem.at[i],
            device_id=device,
            device_id_type=pl.DeviceIdType.MESH,
        )

    def along(h):
        return (x, y) if h == 0 else (y, x)

    def block(h, alpha, beta):
        return beta * 4 + alpha if h == 0 else alpha * 4 + beta

    def first(h, s):
        return {"shard_1": shifted(x, SIGN[s], 4)} if h == 0 else {"shard_0": shifted(y, SIGN[s], 4)}

    def second(h, s):
        return first(1 - h, s)

    def part(p):
        return pl.ds(p * part_rows, part_rows)

    def gather1(h, s, t, arriving=False):
        alpha, beta = along(h)
        back = (1 if t == "w" else 0) + (1 if arriving else 0)
        p = 1 - s if t == "o" else s
        ref = rows.at[h, block(h, shifted(alpha, -SIGN[s] * back, 4), beta), part(p)]
        return remote(("a1", h, s, t), ref, ref, first(h, s))

    def gather2(h, s, k, t, arriving=False):
        alpha, beta = along(h)
        back = (1 if t == "w" else 0) + (1 if arriving else 0)
        p = 1 - s if t == "o" else s
        ref = rows.at[
            h, block(h, shifted(alpha, k, 4), shifted(beta, -SIGN[s] * back, 4)), part(p)
        ]
        return remote(("a2", h, s, k, t), ref, ref, second(h, s))

    def reduce1(h, s, k, t):
        alpha, beta = along(h)
        a = shifted(alpha, k, 4)
        if t == "f":
            src = terms.at[h, block(h, a, shifted(beta, 2, 4)), part(s)]
            dst = far1.at[h, s, k]
        else:
            p = 1 - s if t == "o" else s
            src = terms.at[h, block(h, a, shifted(beta, SIGN[s], 4)), part(p)]
            dst = near1.at[h, s, k, part(p)]
        return remote(("r1", h, s, k, t), src, dst, second(h, s))

    def reduce2(h, s, t):
        alpha, beta = along(h)
        if t == "f":
            src = terms.at[h, block(h, shifted(alpha, 2, 4), beta), part(s)]
            dst = far2.at[h, s]
        else:
            p = 1 - s if t == "o" else s
            src = terms.at[h, block(h, shifted(alpha, SIGN[s], 4), beta), part(p)]
            dst = near2.at[h, s, part(p)]
        return remote(("r2", h, s, t), src, dst, first(h, s))

    def slots_of(device, core):
        return pl.ds(pl.multiple_of(core * 64 + device * cap, cap), cap)

    def spread(dz, dc):
        e = shifted(z, dz, 4)
        core = shifted(c, dc, 2)
        return remote(
            ("zi", dz, dc),
            outgoing.at[core, :, pl.ds(pl.multiple_of(e * cap, cap), cap), :],
            rows.at[:, here, slots_of(z, c), :],
            {"expert": e, "shard_2": core},
        )

    def bring(dz, dc):
        j = shifted(z, dz, 4)
        core = shifted(c, dc, 2)
        return remote(
            ("zo", dz, dc),
            terms.at[:, here, slots_of(j, core), :],
            returned.at[c, :, pl.ds(pl.multiple_of(z * cap, cap), cap), :],
            {"expert": j, "shard_2": core},
        )

    partner = {"shard_2": other}

    def aside1(h, o):
        return {"shard_1": shifted(x, o, 4)} if h == 0 else {"shard_0": shifted(y, o, 4)}

    def aside2(h, o):
        return aside1(1 - h, o)

    def block_out():
        at = here * (1 - c) + (x * 4 + y) * c
        return Together(
            remote(("ib",), block_ids, plane_ids.at[c, at], partner),
            remote(("fb",), block_f.at[other], plane_f.at[c, at], partner),
        )

    block_own = pltpu.make_async_copy(
        block_f.at[c], plane_f.at[c, here * (1 - c) + (x * 4 + y) * c], local_sem.at[7]
    )

    ids_own = pltpu.make_async_copy(
        block_ids, plane_ids.at[c, here * (1 - c) + (x * 4 + y) * c], local_sem.at[20]
    )

    def plane1(h, o):
        alpha, beta = along(h)
        ids, ref = plane_ids.at[h, beta * 4 + alpha], plane_f.at[h, beta * 4 + alpha]
        return Together(
            remote(("i1", h, o), ids, ids, aside1(h, o)),
            remote(("f1", h, o), ref, ref, aside1(h, o)),
        )

    def plane2(h, o):
        alpha, beta = along(h)
        ids, ref = plane_ids.at[h, pl.ds(beta * 4, 4)], plane_f.at[h, pl.ds(beta * 4, 4)]
        return Together(
            remote(("i2", h, o), ids, ids, aside2(h, o)),
            remote(("f2", h, o), ref, ref, aside2(h, o)),
        )

    def group_rows(h, at, j):
        return rows_f.at[at, :, 0, j] if h == 0 else rows_f.at[:, at, 1, j]

    TURN = (0, 1, 3, 2)

    def slots_out(h, n, dz):
        e = shifted(z, dz, 4)
        at = shifted(along(h)[1], TURN[n], 4)
        return remote(
            ("fz", h, n, dz),
            slots_f.at[h, n, :, pl.ds(pl.multiple_of(e * cap, cap), cap), :],
            group_rows(h, at, z),
            {"expert": e},
        )

    def slots_own(h, n):
        at = shifted(along(h)[1], TURN[n], 4)
        return pltpu.make_async_copy(
            slots_f.at[h, n, :, pl.ds(pl.multiple_of(z * cap, cap), cap), :],
            group_rows(h, at, z),
            local_sem.at[8 + h * 4 + n],
        )

    def picked_of(h, at):
        ids = plane_ids[h, at].astype(F32)
        return picked(ids[0:1, 0:tokens], ids[1:2, 0:tokens], cap)

    def make_slots(h, n):
        at = shifted(along(h)[1], TURN[n], 4)

        @pl.loop(0, 4)
        def _(i):
            slots_f[h, n, i] = jnp.dot(
                picked_of(h, at * 4 + i), plane_f[h, at * 4 + i], preferred_element_type=F32
            ).astype(BF16)

        for dz in (2, 1, 3):
            slots_out(h, n, dz).start()
        slots_own(h, n).start()

    def terms_out(g, dz):
        j = shifted(z, dz, 4)
        return remote(
            ("ft", g, dz), terms_f.at[g, :, :, j], crossed_f.at[z, g], {"expert": j}
        )

    terms_own = pltpu.make_async_copy(terms_f.at[:, :, :, z], crossed_f.at[z], local_sem.at[16])

    def make_totals():
        for h in (0, 1):
            @pl.loop(0, 16)
            def _(i):
                one, two = i // 4, i % 4
                held = crossed_f[:, one, two, 0] if h == 0 else crossed_f[:, two, one, 1]
                totals_f[h, i] = lax.dot_general(
                    picked_of(h, i), held.reshape(4 * cap, wide_f),
                    (((0,), (0,)), ((), ())), preferred_element_type=F32,
                ).astype(BF16)

    def back1(h, o):
        alpha, beta = along(h)
        return remote(
            ("b1", h, o), totals_f.at[h, pl.ds(shifted(beta, o, 4) * 4, 4)],
            sums1_f.at[h, o - 1], aside2(h, o),
        )

    def back2(h, o):
        alpha, beta = along(h)
        return remote(
            ("b2", h, o), totals_f.at[h, beta * 4 + shifted(alpha, o, 4)],
            sums2_f.at[h, o - 1], aside1(h, o),
        )

    def last_out():
        return remote(("fl",), last_f.at[other], summed.at[c], partner)

    last_own = pltpu.make_async_copy(last_f.at[c], summed.at[c], local_sem.at[17])
    around = [(h, o) for o in (2, 1, 3) for h in (0, 1)]

    def weight_out(which):
        ref = (wg_ref, wu_ref)[which]
        return remote(
            ("w", which),
            ref.at[0, pl.ds(pl.multiple_of(other * half, half), half), :],
            weights.at[:, pl.ds(2 * units + which * units, units)],
            partner,
        )

    def weight_in(which):
        ref = (wg_ref, wu_ref)[which]
        return pltpu.make_async_copy(
            ref.at[0, pl.ds(pl.multiple_of(c * half, half), half), :],
            weights.at[:, pl.ds(which * units, units)],
            local_sem.at[which],
        )

    def pre_in(which):
        ref = (gate_ref, up_ref, hid_ref)[which]
        return pltpu.make_async_copy(ref.at[0], pre.at[which], local_sem.at[2 + which])

    def grads_out():
        return remote(
            ("g",), grads.at[:, pl.ds(0, 2 * units)], grads.at[:, pl.ds(2 * units, 2 * units)], partner
        )

    own_in = pltpu.make_async_copy(
        outgoing.at[c, :, pl.ds(pl.multiple_of(z * cap, cap), cap), :],
        rows.at[:, here, slots_of(z, c), :],
        local_sem.at[5],
    )

    own_out = pltpu.make_async_copy(
        terms.at[:, here, slots_of(z, c), :],
        returned.at[c, :, pl.ds(pl.multiple_of(z * cap, cap), cap), :],
        local_sem.at[6],
    )

    peers = [(dz, dc) for dz in (2, 1, 3, 0) for dc in (0, 1) if (dz, dc) != (0, 0)]
    both = [(h, s) for h in (0, 1) for s in (0, 1)]

    ids_in = pltpu.make_async_copy(ids_any, ids_t_ref, local_sem.at[18])
    tok_in = pltpu.make_async_copy(tok_any, tok_ref, local_sem.at[19])
    ids_in.start()
    tok_in.start()
    for which in range(3):
        pre_in(which).start()
    for which in range(2):
        weight_in(which).start()
    barrier = pltpu.get_barrier_semaphore()
    for dz, dc in peers:
        pl.semaphore_signal(
            barrier, inc=1,
            device_id={"expert": shifted(z, dz, 4), "shard_2": shifted(c, dc, 2)},
            device_id_type=pl.DeviceIdType.MESH,
        )
    for h, s in both:
        pl.semaphore_signal(
            barrier, inc=1, device_id=first(h, s), device_id_type=pl.DeviceIdType.MESH
        )
    for h in (0, 1):
        pl.semaphore_signal(
            barrier, inc=1, device_id=aside1(h, 2), device_id_type=pl.DeviceIdType.MESH
        )

    ids_in.wait()
    tok_in.wait()
    ids = ids_t_ref[...].astype(F32)
    pick_t = picked(ids[0:1, :], ids[1:2, :], cap)
    for core in range(2):
        at = core * half + 2 * quarter
        block_f[core] = tok_ref[:, at:at + wide_f]
    block_ids[...] = jnp.zeros(block_ids.shape, BF16)
    block_ids[0:2, 0:tokens] = ids.astype(BF16)
    for core in range(2):
        for h in range(2):
            at = core * half + h * quarter
            outgoing[core, h] = jnp.dot(
                pick_t, tok_ref[:, at:at + quarter], preferred_element_type=F32
            ).astype(BF16)

    pl.semaphore_wait(barrier, len(peers) + len(both) + 2)
    block_out().start()
    block_own.start()
    ids_own.start()
    for dz, dc in peers:
        spread(dz, dc).start()
    own_in.start()
    block_own.wait()
    ids_own.wait()
    block_out().wait_recv()
    for h, o in around:
        plane1(h, o).start()

    for which in range(2):
        weight_out(which).start()

    for which in range(3):
        pre_in(which).wait()

    pieces = pre.shape[1] // 64

    def make_grads(i):
        at = pl.ds(pl.multiple_of(i * 64, 64), 64)
        a = pre[0, at, :].astype(F32)
        b = pre[1, at, :].astype(F32)
        g = pre[2, at, :].astype(F32)
        sig = 1.0 / (1.0 + jnp.exp(-a))
        gs = g * sig
        grads[at, 0:units] = (gs * b * (1.0 + a * (1.0 - sig))).astype(BF16)
        grads[at, units:2 * units] = (gs * a).astype(BF16)

    pl.loop(0, pieces // 2)(make_grads)
    for h, o in around:
        plane1(h, o).wait_recv()
    for h, o in around:
        plane2(h, o).start()
    pl.loop(pieces // 2, pieces)(make_grads)
    grads_out().start()

    own_in.wait()
    for dz, dc in peers:
        spread(dz, dc).wait_recv()
    for t in ("f", "o"):
        for h, s in both:
            gather1(h, s, t).start()
    for t in ("f", "o"):
        for h, s in both:
            gather2(h, s, 0, t).start()

    def send_part(h, k, p):
        for s in ((0, 1) if p == 0 else (1, 0)):
            gather2(h, s, k, "f" if s == p else "o").start()

    def group_stage(n):
        for h in (0, 1):
            if n:
                plane2(h, (None, 3, 1, 2)[n]).wait_recv()
            make_slots(h, n)

    def gather_stage(i):
        if i == 0:
            group_stage(0)
        if i == 1:
            for h, s in both:
                gather1(h, s, "f", True).wait_recv()
                gather1(h, s, "w").start()
            for h in (0, 1):
                send_part(h, 3, 0)
                send_part(h, 1, 1)
        if i == 2:
            for h, s in both:
                gather1(h, s, "o", True).wait_recv()
            for h in (0, 1):
                send_part(h, 3, 1)
                send_part(h, 1, 0)
            for g in range(4):
                for dz in (2, 1, 3):
                    terms_out(g, dz).start()
            terms_own.start()
        if i == 3:
            for h, s in both:
                gather2(h, s, 0, "f", True).wait_recv()
                gather2(h, s, 0, "w").start()
            group_stage(1)
        if i == 4:
            for h, s in both:
                gather1(h, s, "w", True).wait_recv()
            for h in (0, 1):
                gather2(h, 0, 2, "f").start()
                gather2(h, 1, 2, "f").start()
                gather2(h, 0, 2, "o").start()
                gather2(h, 1, 2, "o").start()
            group_stage(2)
        if i == 5:
            for h in (0, 1):
                for s, k in ((0, 3), (1, 1)):
                    gather2(h, s, k, "f", True).wait_recv()
                    gather2(h, s, k, "w").start()
            group_stage(3)
        if i == 6:
            for h in (0, 1):
                for s, k in ((0, 1), (1, 3)):
                    gather2(h, s, k, "f", True).wait_recv()
                    gather2(h, s, k, "w").start()

    for which in range(2):
        weight_in(which).wait()
        weight_out(which).wait_recv()
    grads_out().wait_recv()

    group = 4 * rows.shape[2]

    @pl.loop(0, 8)
    def _(i):
        for stage in range(7):
            @pl.when(i == stage)
            def _():
                gather_stage(stage)
        tile = (i + 6) % 8

        @pl.loop(0, 4)
        def _(g):
            left = grads[pl.ds(pl.multiple_of(g * group, group), group), :]
            right = weights[pl.ds(pl.multiple_of(tile * 256, 256), 256), :]
            out = lax.dot_general(
                left, right, (((1,), (1,)), ((), ())), preferred_element_type=F32
            ).astype(BF16)

            @pl.when(tile < 6)
            def _():
                terms[
                    tile // 3, pl.ds(g * 4, 4), :, pl.ds(pl.multiple_of(tile % 3 * 256, 256), 256)
                ] = out.reshape(4, rows.shape[2], 256)

            for m in range(2):
                @pl.when(tile == 6 + m)
                def _():
                    terms_f[g, :, :, :, :, m * 256:(m + 1) * 256] = out.reshape(4, 2, 4, cap, 256)

    for h, s in both:
        gather2(h, s, 2, "f", True).wait_recv()
        gather2(h, s, 2, "w").start()

    for k, t in ((2, "f"), (1, "f"), (2, "o"), (3, "f")):
        for h, s in both:
            reduce1(h, s, k, t).start()

    for h, s in both:
        for k in (0, 1, 3, 2):
            gather2(h, s, k, "o", True).wait_recv()
            gather2(h, s, k, "w", True).wait_recv()

    def add_into(h, at, p, sources):
        @pl.loop(0, part_rows // 16)
        def _(i):
            lines = pl.ds(pl.multiple_of(p * part_rows + i * 16, 16), 16)
            total = terms[h, at, lines, :].astype(F32)
            for ref, base in sources:
                total = total + ref[
                    pl.ds(pl.multiple_of(base + i * 16, 16), 16), :
                ].astype(F32)
            terms[h, at, lines, :] = total.astype(BF16)

    def relay1(k):
        for h, s in both:
            reduce1(h, s, k, "f").wait_recv()
            alpha, beta = along(h)
            add_into(
                h, block(h, shifted(alpha, k, 4), shifted(beta, SIGN[s], 4)), s,
                [(far1.at[h, s, k], 0)],
            )
            reduce1(h, s, k, "w").start()

    def finish1(k):
        for h in (0, 1):
            for s in (0, 1):
                reduce1(h, s, k, "o").wait_recv()
                reduce1(h, s, k, "w").wait_recv()
            alpha, beta = along(h)
            for p in (0, 1):
                base = p * part_rows
                add_into(
                    h, block(h, shifted(alpha, k, 4), beta), p,
                    [(near1.at[h, 0, k], base), (near1.at[h, 1, k], base)],
                )

    def send1(k, t):
        for h, s in both:
            reduce1(h, s, k, t).start()

    def reduce_stage(i):
        if i == 1:
            relay1(2)
            send1(1, "o")
        if i == 2:
            relay1(1)
            send1(3, "o")
        if i == 3:
            relay1(3)
            send1(0, "f")
        if i == 4:
            finish1(2)
            for h, s in both:
                reduce2(h, s, "f").start()
            send1(0, "o")
        if i == 5:
            terms_own.wait()
            for g in range(4):
                for dz in (2, 1, 3):
                    terms_out(g, dz).wait_recv()
            make_totals()
        if i == 6:
            finish1(1)
            finish1(3)
            for h, s in both:
                reduce2(h, s, "o").start()
            relay1(0)
        if i == 7:
            for h, s in both:
                reduce2(h, s, "f").wait_recv()
                alpha, beta = along(h)
                add_into(h, block(h, shifted(alpha, SIGN[s], 4), beta), s, [(far2.at[h, s], 0)])
                reduce2(h, s, "w").start()
            for h, o in around:
                back1(h, o).start()

    def out_rows(i):
        at = pl.multiple_of(c * half + i * 256, 256)
        return pl.ds(at, 256)

    def out_local(i, which):
        return pltpu.make_async_copy(
            staged.at[i, which], (og_ref, ou_ref)[which].at[0, out_rows(i), :], out_sem.at[i, which]
        )

    def out_remote(i, which):
        return pltpu.make_async_remote_copy(
            src_ref=staged.at[i, 2 + which],
            dst_ref=(og_ref, ou_ref)[which].at[0, out_rows(i), :],
            send_sem=out_send.at[i, which],
            recv_sem=out_recv.at[i, which],
            device_id=partner,
            device_id_type=pl.DeviceIdType.MESH,
        )

    all_rows = rows.shape[1] * rows.shape[2]

    @pl.loop(0, 8)
    def _(i):
        for stage in range(1, 8):
            @pl.when(i == stage)
            def _():
                reduce_stage(stage)
        def multiply(left):
            for q in range(4):
                staged[i, q] = lax.dot_general(
                    left, grads[:, q * units:(q + 1) * units], (((0,), (0,)), ((), ())),
                    preferred_element_type=F32,
                )

        @pl.when(i < 6)
        def _():
            at = pl.ds(pl.multiple_of(i % 3 * 256, 256), 256)
            multiply(rows[i // 3, :, :, at].reshape(all_rows, 256))

        @pl.when(i == 6)
        def _():
            for h in (0, 1):
                for n in range(4):
                    for dz in (2, 1, 3):
                        slots_out(h, n, dz).wait_recv()
                    slots_own(h, n).wait()

        @pl.when(i >= 6)
        def _():
            at = pl.ds(pl.multiple_of((i - 6) % 2 * 256, 256), 256)
            multiply(rows_f[:, :, :, :, :, at].reshape(all_rows, 256))

        for which in range(2):
            out_local(i, which).start()
            out_remote(i, which).start()

    finish1(0)
    for h, s in both:
        reduce2(h, s, "o").wait_recv()
        reduce2(h, s, "w").wait_recv()
    for h in (0, 1):
        for p in (0, 1):
            base = p * part_rows
            add_into(h, here, p, [(near2.at[h, 0], base), (near2.at[h, 1], base)])

    for dz, dc in peers:
        bring(dz, dc).start()
    own_out.start()

    for h in (0, 1):
        for o in (1, 2, 3):
            back1(h, o).wait_recv()
        base = along(h)[1] * 4

        @pl.loop(0, 4)
        def _(i):
            total = totals_f[h, base + i].astype(F32)
            for o in range(3):
                total = total + sums1_f[h, o, i].astype(F32)
            totals_f[h, base + i] = total.astype(BF16)

        for o in (2, 1, 3):
            back2(h, o).start()


    for h in (0, 1):
        for o in (1, 2, 3):
            back2(h, o).wait_recv()
        alpha, beta = along(h)
        total = totals_f[h, beta * 4 + alpha].astype(F32)
        for o in range(3):
            total = total + sums2_f[h, o].astype(F32)
        last_f[h] = total.astype(BF16)
    last_out().start()
    last_own.start()
    last_own.wait()
    last_out().wait_recv()
    own_out.wait()
    for dz, dc in peers:
        bring(dz, dc).wait_recv()
    for dz, dc in peers:
        spread(dz, dc).wait_send()
        bring(dz, dc).wait_send()
    for which in range(2):
        weight_out(which).wait_send()
    grads_out().wait_send()
    block_out().wait_send()
    last_out().wait_send()
    for h, o in around:
        plane1(h, o).wait_send()
        plane2(h, o).wait_send()
        back1(h, o).wait_send()
        back2(h, o).wait_send()
    for h in (0, 1):
        for n in range(4):
            for dz in (2, 1, 3):
                slots_out(h, n, dz).wait_send()
    for g in range(4):
        for dz in (2, 1, 3):
            terms_out(g, dz).wait_send()
    for h, s in both:
        for t in ("f", "o", "w"):
            gather1(h, s, t).wait_send()
            reduce2(h, s, t).wait_send()
            for k in range(4):
                gather2(h, s, k, t).wait_send()
                reduce1(h, s, k, t).wait_send()

    @pl.loop(0, 8)
    def _(i):
        for which in range(2):
            out_local(i, which).wait()
            out_remote(i, which).wait()


MESSAGES = 7 + 7 + 2 + 1 + 12 + 48 + 48 + 12 + 1 + 1 + 4 * 6 + 24 + 12 + 13


def on_device(tokens, expert_ids, weight_gate, weight_up, gate_pre, up_pre, hidden_grad):
    count, width = tokens.shape
    slots, units = gate_pre.shape[1:]
    wide_f = width // 8
    quarter = (width // 2 - wide_f) // 2
    lines = slots // 16
    vmem = pl.BlockSpec(memory_space=pltpu.VMEM)
    anywhere = pl.BlockSpec(memory_space=pl.ANY)
    dma = pltpu.SemaphoreType.DMA
    ids_t = expert_ids.T
    returned, summed, gate_out, up_out = pl.pallas_call(
        kernel,
        out_shape=(
            pltpu.VMEM((2, 2, 64, quarter), BF16),
            pltpu.VMEM((2, count, wide_f), BF16),
            pltpu.VMEM((1, width, units), F32),
            pltpu.VMEM((1, width, units), F32),
        ),
        in_specs=[anywhere] * 7,
        out_specs=(anywhere,) * 4,
        scratch_shapes=[
            pltpu.VMEM((2, 16, lines, quarter), BF16),
            pltpu.VMEM((4, 4, 2, 4, 16, wide_f), BF16),
            pltpu.VMEM((slots, 4 * units), BF16),
            pltpu.VMEM((width // 2, 4 * units), BF16),
            pltpu.VMEM((2, 16, lines, quarter), BF16),
            pltpu.VMEM((4, 4, 2, 4, 16, wide_f), BF16),
            pltpu.VMEM((2, 2, 4, lines, quarter), BF16),
            pltpu.VMEM((2, 2, 4, lines // 2, quarter), BF16),
            pltpu.VMEM((2, 2, lines, quarter), BF16),
            pltpu.VMEM((2, 2, lines // 2, quarter), BF16),
            pltpu.VMEM((8, 4, 256, units), F32),
            pltpu.VMEM((3, slots, units), BF16),
            pltpu.VMEM((2, 2, 64, quarter), BF16),
            pltpu.VMEM((2, count, wide_f), BF16),
            pltpu.VMEM((2, 16, count, wide_f), BF16),
            pltpu.VMEM((2, 4, 4, 64, wide_f), BF16),
            pltpu.VMEM((4, 4, 4, 2, 16, wide_f), BF16),
            pltpu.VMEM((2, 16, count, wide_f), BF16),
            pltpu.VMEM((2, 3, 4, count, wide_f), BF16),
            pltpu.VMEM((2, 3, count, wide_f), BF16),
            pltpu.VMEM((2, count, wide_f), BF16),
            pltpu.VMEM(expert_ids.shape[::-1], jnp.int32),
            pltpu.VMEM((count, width), BF16),
            pltpu.VMEM((8, 128), BF16),
            pltpu.VMEM((2, 16, 8, 128), BF16),
            dma((MESSAGES,)),
            dma((MESSAGES,)),
            dma((21,)),
            dma((8, 2)),
            dma((8, 2)),
            dma((8, 2)),
        ],
        compiler_params=pltpu.CompilerParams(
            collective_id=0, has_side_effects=True, vmem_limit_bytes=51 * 1024 * 1024
        ),
    )(ids_t, tokens, weight_gate, weight_up, gate_pre, up_pre, hidden_grad)
    return pl.pallas_call(
        finish,
        out_shape=(
            jax.ShapeDtypeStruct((count, width), BF16),
            jax.ShapeDtypeStruct((1, width, units), F32),
            jax.ShapeDtypeStruct((1, width, units), F32),
        ),
        in_specs=[vmem, vmem, vmem, anywhere, anywhere],
        out_specs=(anywhere,) * 3,
        scratch_shapes=[pltpu.VMEM((count, width), BF16), dma((9,))],
        compiler_params=pltpu.CompilerParams(vmem_limit_bytes=8 * 1024 * 1024),
    )(ids_t, returned, summed, gate_out, up_out)


def solution(mesh):
    torus = Mesh(
        mesh.devices.reshape(mesh.shape["expert"], 4, 4, 2),
        ("expert", "shard_0", "shard_1", "shard_2"),
    )
    split = P("expert", None, SHARD)
    placed = (P(EXPERT_SHARD, None), P(EXPERT_SHARD, None), split, split, split, split, split)
    return jax.shard_map(
        on_device,
        mesh=torus,
        in_specs=placed,
        out_specs=(P(EXPERT_SHARD, None), split, split),
        check_vma=False,
    )
```

```python
import functools

import jax
import jax.numpy as jnp
from jax import lax
from jax.experimental import pallas as pl
from jax.experimental.pallas import tpu as pltpu
from jax.sharding import Mesh
from jax.sharding import PartitionSpec as P

SHARD = ("shard_0", "shard_1", "shard_2")
EXPERT_SHARD = ("expert", "shard_0", "shard_1", "shard_2")
SIGN = (1, -1)
F32 = jnp.float32
BF16 = jnp.bfloat16


def shifted(value, by, size):
    return lax.rem(value + by % size, size)


def picked(first_ids, second_ids, cap):
    tokens = first_ids.shape[1]
    line = lax.broadcasted_iota(jnp.int32, (4 * cap, tokens), 0)
    expert = (line // cap).astype(F32)
    named = (first_ids == expert) | (second_ids == expert)
    before = (
        lax.broadcasted_iota(jnp.int32, (tokens, tokens), 0)
        < lax.broadcasted_iota(jnp.int32, (tokens, tokens), 1)
    )
    slot = jnp.dot(
        named.astype(F32).astype(BF16), before.astype(F32).astype(BF16), preferred_element_type=F32
    )
    return jnp.where(named & (slot == (line % cap).astype(F32)), 1.0, 0.0).astype(BF16)


def finish(ids_t_ref, returned, summed, og_in, ou_in, tg_out, og_ref, ou_ref, tg_ref, sems):
    width = og_in.shape[1] // 4

    def put(i):
        which, q = i // 4, i % 4
        at = pl.ds(q * width, width)
        return pltpu.make_async_copy(
            (og_in, ou_in)[which].at[0, at, :], (og_ref, ou_ref)[which].at[0, at, :], sems.at[i]
        )

    for i in range(8):
        put(i).start()
    ids = ids_t_ref[...].astype(F32)
    pick_t = picked(ids[0:1, :], ids[1:2, :], 16)
    tokens = tg_ref.shape[0]
    half = tg_ref.shape[1] // 2
    quarter = returned.shape[3]
    for core in range(2):
        for h in range(2):
            at = core * half + h * quarter
            tg_ref[:, at:at + quarter] = lax.dot_general(
                pick_t, returned[core, h], (((0,), (0,)), ((), ())), preferred_element_type=F32
            ).astype(BF16)
        at = core * half + 2 * quarter
        tg_ref[:, at:(core + 1) * half] = summed[core]
    tg_copy = pltpu.make_async_copy(tg_ref, tg_out, sems.at[8])
    tg_copy.start()
    for i in range(8):
        put(i).wait()
    tg_copy.wait()


class Together:
    def __init__(self, *copies):
        self.copies = copies

    def start(self):
        for copy in self.copies:
            copy.start()

    def wait_recv(self):
        for copy in self.copies:
            copy.wait_recv()

    def wait_send(self):
        for copy in self.copies:
            copy.wait_send()


def kernel(
    ids_any, tok_any, wg_ref, wu_ref, gate_ref, up_ref, hid_ref,
    returned, summed, og_ref, ou_ref,
    rows, rows_f, grads, weights, terms, terms_f, near1, far1, near2, far2, staged, pre, outgoing,
    block_f, plane_f, slots_f, crossed_f, totals_f, sums1_f, sums2_f, last_f,
    ids_t_ref, tok_ref, block_ids, plane_ids,
    send_sem, recv_sem, local_sem, out_sem, out_send, out_recv,
):
    z = lax.axis_index("expert")
    y = lax.axis_index("shard_0")
    x = lax.axis_index("shard_1")
    c = lax.axis_index("shard_2")
    other = 1 - c
    here = y * 4 + x
    half = tok_ref.shape[1] // 2
    quarter = rows.shape[3]
    wide_f = rows_f.shape[5]
    units = gate_ref.shape[2]
    tokens = tok_ref.shape[0]
    cap = 16
    part_rows = rows.shape[2] // 2

    numbers = {}

    def number(key):
        return numbers.setdefault(key, len(numbers))

    def remote(key, src, dst, device):
        i = number(key)
        return pltpu.make_async_remote_copy(
            src_ref=src,
            dst_ref=dst,
            send_sem=send_sem.at[i],
            recv_sem=recv_sem.at[i],
            device_id=device,
            device_id_type=pl.DeviceIdType.MESH,
        )

    def along(h):
        return (x, y) if h == 0 else (y, x)

    def block(h, alpha, beta):
        return beta * 4 + alpha if h == 0 else alpha * 4 + beta

    def first(h, s):
        return {"shard_1": shifted(x, SIGN[s], 4)} if h == 0 else {"shard_0": shifted(y, SIGN[s], 4)}

    def second(h, s):
        return first(1 - h, s)

    def part(p):
        return pl.ds(p * part_rows, part_rows)

    def quarter_of(p, dz):
        if dz is None:
            return part(p)
        return pl.ds(pl.multiple_of(p * part_rows + shifted(z, dz, 4) * cap, cap), cap)

    def gather1(h, s, t, arriving=False, dz=None):
        alpha, beta = along(h)
        back = (1 if t == "w" else 0) + (1 if arriving else 0)
        p = 1 - s if t == "o" else s
        at = block(h, shifted(alpha, -SIGN[s] * back, 4), beta)
        ref = rows.at[h, at, quarter_of(p, dz)]
        return remote(("a1", h, s, t, dz), ref, ref, first(h, s))

    def gather2(h, s, k, t, arriving=False, dz=None):
        alpha, beta = along(h)
        back = (1 if t == "w" else 0) + (1 if arriving else 0)
        p = 1 - s if t == "o" else s
        at = block(h, shifted(alpha, k, 4), shifted(beta, -SIGN[s] * back, 4))
        ref = rows.at[h, at, quarter_of(p, dz)]
        return remote(("a2", h, s, k, t, dz), ref, ref, second(h, s))

    def send_own(dz):
        for t in ("f", "o"):
            for h, s in both:
                gather1(h, s, t, dz=dz).start()
        for t in ("f", "o"):
            for h, s in both:
                gather2(h, s, 0, t, dz=dz).start()

    def got1(h, s, t):
        for dz in range(4):
            gather1(h, s, t, True, dz).wait_recv()

    def got2(h, s, t):
        for dz in range(4):
            gather2(h, s, 0, t, True, dz).wait_recv()

    def reduce1(h, s, k, t):
        alpha, beta = along(h)
        a = shifted(alpha, k, 4)
        if t == "f":
            src = terms.at[h, block(h, a, shifted(beta, 2, 4)), part(s)]
            dst = far1.at[h, s, k]
        else:
            p = 1 - s if t == "o" else s
            src = terms.at[h, block(h, a, shifted(beta, SIGN[s], 4)), part(p)]
            dst = near1.at[h, s, k, part(p)]
        return remote(("r1", h, s, k, t), src, dst, second(h, s))

    def reduce2(h, s, t):
        alpha, beta = along(h)
        if t == "f":
            src = terms.at[h, block(h, shifted(alpha, 2, 4), beta), part(s)]
            dst = far2.at[h, s]
        else:
            p = 1 - s if t == "o" else s
            src = terms.at[h, block(h, shifted(alpha, SIGN[s], 4), beta), part(p)]
            dst = near2.at[h, s, part(p)]
        return remote(("r2", h, s, t), src, dst, first(h, s))

    def slots_of(device, core):
        return pl.ds(pl.multiple_of(core * 64 + device * cap, cap), cap)

    def spread(dz, dc):
        e = shifted(z, dz, 4)
        core = shifted(c, dc, 2)
        return remote(
            ("zi", dz, dc),
            outgoing.at[core, :, pl.ds(pl.multiple_of(e * cap, cap), cap), :],
            rows.at[:, here, slots_of(z, c), :],
            {"expert": e, "shard_2": core},
        )

    def bring(dz, dc):
        j = shifted(z, dz, 4)
        core = shifted(c, dc, 2)
        return remote(
            ("zo", dz, dc),
            terms.at[:, here, slots_of(j, core), :],
            returned.at[c, :, pl.ds(pl.multiple_of(z * cap, cap), cap), :],
            {"expert": j, "shard_2": core},
        )

    partner = {"shard_2": other}

    def aside1(h, o):
        return {"shard_1": shifted(x, o, 4)} if h == 0 else {"shard_0": shifted(y, o, 4)}

    def aside2(h, o):
        return aside1(1 - h, o)

    def block_out():
        at = here * (1 - c) + (x * 4 + y) * c
        return Together(
            remote(("ib",), block_ids, plane_ids.at[c, at], partner),
            remote(("fb",), block_f.at[other], plane_f.at[c, at], partner),
        )

    block_own = pltpu.make_async_copy(
        block_f.at[c], plane_f.at[c, here * (1 - c) + (x * 4 + y) * c], local_sem.at[7]
    )

    ids_own = pltpu.make_async_copy(
        block_ids, plane_ids.at[c, here * (1 - c) + (x * 4 + y) * c], local_sem.at[20]
    )

    def plane1(h, o):
        alpha, beta = along(h)
        ids, ref = plane_ids.at[h, beta * 4 + alpha], plane_f.at[h, beta * 4 + alpha]
        return Together(
            remote(("i1", h, o), ids, ids, aside1(h, o)),
            remote(("f1", h, o), ref, ref, aside1(h, o)),
        )

    def plane2(h, o):
        alpha, beta = along(h)
        ids, ref = plane_ids.at[h, pl.ds(beta * 4, 4)], plane_f.at[h, pl.ds(beta * 4, 4)]
        return Together(
            remote(("i2", h, o), ids, ids, aside2(h, o)),
            remote(("f2", h, o), ref, ref, aside2(h, o)),
        )

    def group_rows(h, at, j):
        return rows_f.at[at, :, 0, j] if h == 0 else rows_f.at[:, at, 1, j]

    TURN = (0, 1, 3, 2)

    def slots_out(h, n, dz):
        e = shifted(z, dz, 4)
        at = shifted(along(h)[1], TURN[n], 4)
        return remote(
            ("fz", h, n, dz),
            slots_f.at[h, n, :, pl.ds(pl.multiple_of(e * cap, cap), cap), :],
            group_rows(h, at, z),
            {"expert": e},
        )

    def slots_own(h, n):
        at = shifted(along(h)[1], TURN[n], 4)
        return pltpu.make_async_copy(
            slots_f.at[h, n, :, pl.ds(pl.multiple_of(z * cap, cap), cap), :],
            group_rows(h, at, z),
            local_sem.at[8 + h * 4 + n],
        )

    def picked_of(h, at):
        ids = plane_ids[h, at].astype(F32)
        return picked(ids[0:1, 0:tokens], ids[1:2, 0:tokens], cap)

    def make_slots(h, n):
        at = shifted(along(h)[1], TURN[n], 4)

        @pl.loop(0, 4)
        def _(i):
            slots_f[h, n, i] = jnp.dot(
                picked_of(h, at * 4 + i), plane_f[h, at * 4 + i], preferred_element_type=F32
            ).astype(BF16)

        for dz in (2, 1, 3):
            slots_out(h, n, dz).start()
        slots_own(h, n).start()

    def terms_out(g, dz):
        j = shifted(z, dz, 4)
        return remote(
            ("ft", g, dz), terms_f.at[g, :, :, j], crossed_f.at[z, g], {"expert": j}
        )

    terms_own = pltpu.make_async_copy(terms_f.at[:, :, :, z], crossed_f.at[z], local_sem.at[16])

    def make_totals():
        for h in (0, 1):
            @pl.loop(0, 16)
            def _(i):
                one, two = i // 4, i % 4
                held = crossed_f[:, one, two, 0] if h == 0 else crossed_f[:, two, one, 1]
                totals_f[h, i] = lax.dot_general(
                    picked_of(h, i), held.reshape(4 * cap, wide_f),
                    (((0,), (0,)), ((), ())), preferred_element_type=F32,
                ).astype(BF16)

    def back1(h, o):
        alpha, beta = along(h)
        return remote(
            ("b1", h, o), totals_f.at[h, pl.ds(shifted(beta, o, 4) * 4, 4)],
            sums1_f.at[h, o - 1], aside2(h, o),
        )

    def back2(h, o):
        alpha, beta = along(h)
        return remote(
            ("b2", h, o), totals_f.at[h, beta * 4 + shifted(alpha, o, 4)],
            sums2_f.at[h, o - 1], aside1(h, o),
        )

    def last_out():
        return remote(("fl",), last_f.at[other], summed.at[c], partner)

    last_own = pltpu.make_async_copy(last_f.at[c], summed.at[c], local_sem.at[17])
    around = [(h, o) for o in (2, 1, 3) for h in (0, 1)]

    def weight_out(which):
        ref = (wg_ref, wu_ref)[which]
        return remote(
            ("w", which),
            ref.at[0, pl.ds(pl.multiple_of(other * half, half), half), :],
            weights.at[:, pl.ds(2 * units + which * units, units)],
            partner,
        )

    def weight_in(which):
        ref = (wg_ref, wu_ref)[which]
        return pltpu.make_async_copy(
            ref.at[0, pl.ds(pl.multiple_of(c * half, half), half), :],
            weights.at[:, pl.ds(which * units, units)],
            local_sem.at[which],
        )

    def pre_in(which):
        ref = (gate_ref, up_ref, hid_ref)[which]
        return pltpu.make_async_copy(ref.at[0], pre.at[which], local_sem.at[2 + which])

    def grads_out():
        return remote(
            ("g",), grads.at[:, pl.ds(0, 2 * units)], grads.at[:, pl.ds(2 * units, 2 * units)], partner
        )

    own_in = pltpu.make_async_copy(
        outgoing.at[c, :, pl.ds(pl.multiple_of(z * cap, cap), cap), :],
        rows.at[:, here, slots_of(z, c), :],
        local_sem.at[5],
    )

    own_out = pltpu.make_async_copy(
        terms.at[:, here, slots_of(z, c), :],
        returned.at[c, :, pl.ds(pl.multiple_of(z * cap, cap), cap), :],
        local_sem.at[6],
    )

    peers = [(0, 1)] + [(dz, dc) for dz in (2, 1, 3) for dc in (0, 1)]
    both = [(h, s) for h in (0, 1) for s in (0, 1)]

    ids_in = pltpu.make_async_copy(ids_any, ids_t_ref, local_sem.at[18])
    tok_in = pltpu.make_async_copy(tok_any, tok_ref, local_sem.at[19])
    ids_in.start()
    tok_in.start()
    for which in range(3):
        pre_in(which).start()
    for which in range(2):
        weight_in(which).start()
    barrier = pltpu.get_barrier_semaphore()
    for dz, dc in peers:
        pl.semaphore_signal(
            barrier, inc=1,
            device_id={"expert": shifted(z, dz, 4), "shard_2": shifted(c, dc, 2)},
            device_id_type=pl.DeviceIdType.MESH,
        )
    for h, s in both:
        pl.semaphore_signal(
            barrier, inc=1, device_id=first(h, s), device_id_type=pl.DeviceIdType.MESH
        )
    for h in (0, 1):
        pl.semaphore_signal(
            barrier, inc=1, device_id=aside1(h, 2), device_id_type=pl.DeviceIdType.MESH
        )

    ids_in.wait()
    tok_in.wait()
    ids = ids_t_ref[...].astype(F32)
    pick_t = picked(ids[0:1, :], ids[1:2, :], cap)
    for core in range(2):
        at = core * half + 2 * quarter
        block_f[core] = tok_ref[:, at:at + wide_f]
    block_ids[...] = jnp.zeros(block_ids.shape, BF16)
    block_ids[0:2, 0:tokens] = ids.astype(BF16)
    for core in range(2):
        for h in range(2):
            at = core * half + h * quarter
            outgoing[core, h] = jnp.dot(
                pick_t, tok_ref[:, at:at + quarter], preferred_element_type=F32
            ).astype(BF16)

    pl.semaphore_wait(barrier, len(peers) + len(both) + 2)
    block_out().start()
    block_own.start()
    ids_own.start()
    for dz, dc in peers:
        spread(dz, dc).start()
    own_in.start()
    block_own.wait()
    ids_own.wait()
    block_out().wait_recv()
    for h, o in around:
        plane1(h, o).start()
    own_in.wait()
    spread(0, 1).wait_recv()
    send_own(0)
    for which in range(2):
        weight_out(which).start()

    for which in range(3):
        pre_in(which).wait()

    pieces = pre.shape[1] // 64

    def make_grads(i):
        at = pl.ds(pl.multiple_of(i * 64, 64), 64)
        a = pre[0, at, :].astype(F32)
        b = pre[1, at, :].astype(F32)
        g = pre[2, at, :].astype(F32)
        sig = 1.0 / (1.0 + jnp.exp(-a))
        gs = g * sig
        grads[at, 0:units] = (gs * b * (1.0 + a * (1.0 - sig))).astype(BF16)
        grads[at, units:2 * units] = (gs * a).astype(BF16)

    pl.loop(0, pieces // 2)(make_grads)
    for h, o in around:
        plane1(h, o).wait_recv()
    for h, o in around:
        plane2(h, o).start()
    for dz in (1, 3, 2):
        for dc in (0, 1):
            spread(dz, dc).wait_recv()
        send_own(4 - dz)

    pl.loop(pieces // 2, pieces)(make_grads)
    grads_out().start()

    def send_part(h, k, p):
        for s in ((0, 1) if p == 0 else (1, 0)):
            gather2(h, s, k, "f" if s == p else "o").start()

    def group_stage(n):
        for h in (0, 1):
            if n:
                plane2(h, (None, 3, 1, 2)[n]).wait_recv()
            make_slots(h, n)

    def gather_stage(i):
        if i == 0:
            group_stage(0)
        if i == 1:
            for h, s in both:
                got1(h, s, "f")
                gather1(h, s, "w").start()
            for h in (0, 1):
                send_part(h, 3, 0)
                send_part(h, 1, 1)
        if i == 2:
            for h, s in both:
                got1(h, s, "o")
            for h in (0, 1):
                send_part(h, 3, 1)
                send_part(h, 1, 0)
            for g in range(4):
                for dz in (2, 1, 3):
                    terms_out(g, dz).start()
            terms_own.start()
        if i == 3:
            for h, s in both:
                got2(h, s, "f")
                gather2(h, s, 0, "w").start()
            group_stage(1)
        if i == 4:
            for h, s in both:
                gather1(h, s, "w", True).wait_recv()
            for h in (0, 1):
                gather2(h, 0, 2, "f").start()
                gather2(h, 1, 2, "f").start()
                gather2(h, 0, 2, "o").start()
                gather2(h, 1, 2, "o").start()
            group_stage(2)
        if i == 5:
            for h in (0, 1):
                for s, k in ((0, 3), (1, 1)):
                    gather2(h, s, k, "f", True).wait_recv()
                    gather2(h, s, k, "w").start()
            group_stage(3)
        if i == 6:
            for h in (0, 1):
                for s, k in ((0, 1), (1, 3)):
                    gather2(h, s, k, "f", True).wait_recv()
                    gather2(h, s, k, "w").start()

    for which in range(2):
        weight_in(which).wait()
        weight_out(which).wait_recv()
    grads_out().wait_recv()

    group = 4 * rows.shape[2]

    @pl.loop(0, 8)
    def _(i):
        for stage in range(7):
            @pl.when(i == stage)
            def _():
                gather_stage(stage)
        tile = (i + 6) % 8

        @pl.loop(0, 4)
        def _(g):
            left = grads[pl.ds(pl.multiple_of(g * group, group), group), :]
            right = weights[pl.ds(pl.multiple_of(tile * 256, 256), 256), :]
            out = lax.dot_general(
                left, right, (((1,), (1,)), ((), ())), preferred_element_type=F32
            ).astype(BF16)

            @pl.when(tile < 6)
            def _():
                terms[
                    tile // 3, pl.ds(g * 4, 4), :, pl.ds(pl.multiple_of(tile % 3 * 256, 256), 256)
                ] = out.reshape(4, rows.shape[2], 256)

            for m in range(2):
                @pl.when(tile == 6 + m)
                def _():
                    terms_f[g, :, :, :, :, m * 256:(m + 1) * 256] = out.reshape(4, 2, 4, cap, 256)

    for h, s in both:
        gather2(h, s, 2, "f", True).wait_recv()
        gather2(h, s, 2, "w").start()

    for k, t in ((2, "f"), (1, "f"), (2, "o"), (3, "f")):
        for h, s in both:
            reduce1(h, s, k, t).start()

    for h, s in both:
        for k in (0, 1, 3, 2):
            if k:
                gather2(h, s, k, "o", True).wait_recv()
            else:
                got2(h, s, "o")
            gather2(h, s, k, "w", True).wait_recv()

    def add_into(h, at, p, sources):
        @pl.loop(0, part_rows // 16)
        def _(i):
            lines = pl.ds(pl.multiple_of(p * part_rows + i * 16, 16), 16)
            total = terms[h, at, lines, :].astype(F32)
            for ref, base in sources:
                total = total + ref[
                    pl.ds(pl.multiple_of(base + i * 16, 16), 16), :
                ].astype(F32)
            terms[h, at, lines, :] = total.astype(BF16)

    def relay1(k):
        for h, s in both:
            reduce1(h, s, k, "f").wait_recv()
            alpha, beta = along(h)
            add_into(
                h, block(h, shifted(alpha, k, 4), shifted(beta, SIGN[s], 4)), s,
                [(far1.at[h, s, k], 0)],
            )
            reduce1(h, s, k, "w").start()

    def finish1(k):
        for h in (0, 1):
            for s in (0, 1):
                reduce1(h, s, k, "o").wait_recv()
                reduce1(h, s, k, "w").wait_recv()
            alpha, beta = along(h)
            for p in (0, 1):
                base = p * part_rows
                add_into(
                    h, block(h, shifted(alpha, k, 4), beta), p,
                    [(near1.at[h, 0, k], base), (near1.at[h, 1, k], base)],
                )

    def send1(k, t):
        for h, s in both:
            reduce1(h, s, k, t).start()

    def reduce_stage(i):
        if i == 1:
            relay1(2)
            send1(1, "o")
        if i == 2:
            relay1(1)
            send1(3, "o")
        if i == 3:
            relay1(3)
            send1(0, "f")
        if i == 4:
            finish1(2)
            for h, s in both:
                reduce2(h, s, "f").start()
            send1(0, "o")
        if i == 5:
            terms_own.wait()
            for g in range(4):
                for dz in (2, 1, 3):
                    terms_out(g, dz).wait_recv()
            make_totals()
        if i == 6:
            finish1(1)
            finish1(3)
            for h, s in both:
                reduce2(h, s, "o").start()
            for h, o in around[0:2]:
                back1(h, o).start()
            relay1(0)
        if i == 7:
            for h, s in both:
                reduce2(h, s, "f").wait_recv()
                alpha, beta = along(h)
                add_into(h, block(h, shifted(alpha, SIGN[s], 4), beta), s, [(far2.at[h, s], 0)])
                reduce2(h, s, "w").start()
            for h, o in around[2:]:
                back1(h, o).start()

    def out_rows(i):
        at = pl.multiple_of(c * half + i * 256, 256)
        return pl.ds(at, 256)

    def out_local(i, which):
        return pltpu.make_async_copy(
            staged.at[i, which], (og_ref, ou_ref)[which].at[0, out_rows(i), :], out_sem.at[i, which]
        )

    def out_remote(i, which):
        return pltpu.make_async_remote_copy(
            src_ref=staged.at[i, 2 + which],
            dst_ref=(og_ref, ou_ref)[which].at[0, out_rows(i), :],
            send_sem=out_send.at[i, which],
            recv_sem=out_recv.at[i, which],
            device_id=partner,
            device_id_type=pl.DeviceIdType.MESH,
        )

    all_rows = rows.shape[1] * rows.shape[2]

    @pl.loop(0, 8)
    def _(i):
        for stage in range(1, 8):
            @pl.when(i == stage)
            def _():
                reduce_stage(stage)
        def multiply(left):
            for q in range(4):
                staged[i, q] = lax.dot_general(
                    left, grads[:, q * units:(q + 1) * units], (((0,), (0,)), ((), ())),
                    preferred_element_type=F32,
                )

        @pl.when(i < 6)
        def _():
            at = pl.ds(pl.multiple_of(i % 3 * 256, 256), 256)
            multiply(rows[i // 3, :, :, at].reshape(all_rows, 256))

        @pl.when(i == 6)
        def _():
            for h in (0, 1):
                for n in range(4):
                    for dz in (2, 1, 3):
                        slots_out(h, n, dz).wait_recv()
                    slots_own(h, n).wait()

        @pl.when(i >= 6)
        def _():
            at = pl.ds(pl.multiple_of((i - 6) % 2 * 256, 256), 256)
            multiply(rows_f[:, :, :, :, :, at].reshape(all_rows, 256))

        for which in range(2):
            out_local(i, which).start()
            out_remote(i, which).start()

    finish1(0)
    for h, s in both:
        reduce2(h, s, "o").wait_recv()
        reduce2(h, s, "w").wait_recv()
    for h in (0, 1):
        for p in (0, 1):
            base = p * part_rows
            add_into(h, here, p, [(near2.at[h, 0], base), (near2.at[h, 1], base)])

    for dz, dc in peers:
        bring(dz, dc).start()
    own_out.start()

    for h in (0, 1):
        for o in (1, 2, 3):
            back1(h, o).wait_recv()
        base = along(h)[1] * 4

        @pl.loop(0, 4)
        def _(i):
            total = totals_f[h, base + i].astype(F32)
            for o in range(3):
                total = total + sums1_f[h, o, i].astype(F32)
            totals_f[h, base + i] = total.astype(BF16)

        for o in (2, 1, 3):
            back2(h, o).start()


    for h in (0, 1):
        for o in (1, 2, 3):
            back2(h, o).wait_recv()
        alpha, beta = along(h)
        total = totals_f[h, beta * 4 + alpha].astype(F32)
        for o in range(3):
            total = total + sums2_f[h, o].astype(F32)
        last_f[h] = total.astype(BF16)
    last_out().start()
    last_own.start()
    last_own.wait()
    last_out().wait_recv()
    own_out.wait()
    for dz, dc in peers:
        bring(dz, dc).wait_recv()
    for dz, dc in peers:
        spread(dz, dc).wait_send()
        bring(dz, dc).wait_send()
    for which in range(2):
        weight_out(which).wait_send()
    grads_out().wait_send()
    block_out().wait_send()
    last_out().wait_send()
    for h, o in around:
        plane1(h, o).wait_send()
        plane2(h, o).wait_send()
        back1(h, o).wait_send()
        back2(h, o).wait_send()
    for h in (0, 1):
        for n in range(4):
            for dz in (2, 1, 3):
                slots_out(h, n, dz).wait_send()
    for g in range(4):
        for dz in (2, 1, 3):
            terms_out(g, dz).wait_send()
    for h, s in both:
        for t in ("f", "o", "w"):
            for dz in (None,) if t == "w" else range(4):
                gather1(h, s, t, dz=dz).wait_send()
                gather2(h, s, 0, t, dz=dz).wait_send()
            reduce2(h, s, t).wait_send()
            for k in range(4):
                if k:
                    gather2(h, s, k, t).wait_send()
                reduce1(h, s, k, t).wait_send()

    @pl.loop(0, 8)
    def _(i):
        for which in range(2):
            out_local(i, which).wait()
            out_remote(i, which).wait()


MESSAGES = 7 + 7 + 2 + 1 + 12 + 48 + 48 + 12 + 48 + 1 + 1 + 4 * 6 + 24 + 12 + 13


def on_device(tokens, expert_ids, weight_gate, weight_up, gate_pre, up_pre, hidden_grad):
    count, width = tokens.shape
    slots, units = gate_pre.shape[1:]
    wide_f = width // 8
    quarter = (width // 2 - wide_f) // 2
    lines = slots // 16
    vmem = pl.BlockSpec(memory_space=pltpu.VMEM)
    anywhere = pl.BlockSpec(memory_space=pl.ANY)
    dma = pltpu.SemaphoreType.DMA
    ids_t = expert_ids.T
    returned, summed, gate_out, up_out = pl.pallas_call(
        kernel,
        out_shape=(
            pltpu.VMEM((2, 2, 64, quarter), BF16),
            pltpu.VMEM((2, count, wide_f), BF16),
            pltpu.VMEM((1, width, units), F32),
            pltpu.VMEM((1, width, units), F32),
        ),
        in_specs=[anywhere] * 7,
        out_specs=(anywhere,) * 4,
        scratch_shapes=[
            pltpu.VMEM((2, 16, lines, quarter), BF16),
            pltpu.VMEM((4, 4, 2, 4, 16, wide_f), BF16),
            pltpu.VMEM((slots, 4 * units), BF16),
            pltpu.VMEM((width // 2, 4 * units), BF16),
            pltpu.VMEM((2, 16, lines, quarter), BF16),
            pltpu.VMEM((4, 4, 2, 4, 16, wide_f), BF16),
            pltpu.VMEM((2, 2, 4, lines, quarter), BF16),
            pltpu.VMEM((2, 2, 4, lines // 2, quarter), BF16),
            pltpu.VMEM((2, 2, lines, quarter), BF16),
            pltpu.VMEM((2, 2, lines // 2, quarter), BF16),
            pltpu.VMEM((8, 4, 256, units), F32),
            pltpu.VMEM((3, slots, units), BF16),
            pltpu.VMEM((2, 2, 64, quarter), BF16),
            pltpu.VMEM((2, count, wide_f), BF16),
            pltpu.VMEM((2, 16, count, wide_f), BF16),
            pltpu.VMEM((2, 4, 4, 64, wide_f), BF16),
            pltpu.VMEM((4, 4, 4, 2, 16, wide_f), BF16),
            pltpu.VMEM((2, 16, count, wide_f), BF16),
            pltpu.VMEM((2, 3, 4, count, wide_f), BF16),
            pltpu.VMEM((2, 3, count, wide_f), BF16),
            pltpu.VMEM((2, count, wide_f), BF16),
            pltpu.VMEM(expert_ids.shape[::-1], jnp.int32),
            pltpu.VMEM((count, width), BF16),
            pltpu.VMEM((8, 128), BF16),
            pltpu.VMEM((2, 16, 8, 128), BF16),
            dma((MESSAGES,)),
            dma((MESSAGES,)),
            dma((21,)),
            dma((8, 2)),
            dma((8, 2)),
            dma((8, 2)),
        ],
        compiler_params=pltpu.CompilerParams(
            collective_id=0, has_side_effects=True, vmem_limit_bytes=51 * 1024 * 1024
        ),
    )(ids_t, tokens, weight_gate, weight_up, gate_pre, up_pre, hidden_grad)
    return pl.pallas_call(
        finish,
        out_shape=(
            jax.ShapeDtypeStruct((count, width), BF16),
            jax.ShapeDtypeStruct((1, width, units), F32),
            jax.ShapeDtypeStruct((1, width, units), F32),
        ),
        in_specs=[vmem, vmem, vmem, anywhere, anywhere],
        out_specs=(anywhere,) * 3,
        scratch_shapes=[pltpu.VMEM((count, width), BF16), dma((9,))],
        compiler_params=pltpu.CompilerParams(vmem_limit_bytes=8 * 1024 * 1024),
    )(ids_t, returned, summed, gate_out, up_out)


def solution(mesh):
    torus = Mesh(
        mesh.devices.reshape(mesh.shape["expert"], 4, 4, 2),
        ("expert", "shard_0", "shard_1", "shard_2"),
    )
    split = P("expert", None, SHARD)
    placed = (P(EXPERT_SHARD, None), P(EXPERT_SHARD, None), split, split, split, split, split)
    return jax.shard_map(
        on_device,
        mesh=torus,
        in_specs=placed,
        out_specs=(P(EXPERT_SHARD, None), split, split),
        check_vma=False,
    )
```
